32 devices in a mesh: band: 8 (over z, x), patch: 4 (over y, core).
Axes of the slice: x: 2, y: 2, z: 4, core: 2. Of those that a mesh axis runs over, the one named last changes fastest.
Arguments:
- latents: bfloat16 [8, 10240, 512], P('band', 'patch'), may hold values from -6 to 6
- owners: int32 [16], replicated, may hold values from 0 to 3, as said below
- block_rows: int32 [16, 128], replicated, may hold values from 0 to 2559
- interp_weights: bfloat16 [16, 1024, 128], P('band', 'patch'), may hold values from -0.5 to 0.5
- w_first: bfloat16 [8, 512, 512], P('band'), may hold values from -0.25 to 0.25
- b_first: float32 [8, 512], P('band'), may hold values from -3 to 3
- w_second: bfloat16 [8, 512, 512], P('band'), may hold values from -0.25 to 0.25
- b_second: float32 [8, 512], P('band'), may hold values from -4 to 4
- gain: float32 [8, 512], P('band'), may hold values from 0.1 to 1.9
- w_out: bfloat16 [8, 12, 512], P('band'), may hold values from -0.25 to 0.25
- b_out: float32 [8, 12], P('band'), may hold values from -4 to 4
Outputs:
- grid_fields: float32 [8, 12, 16384], P('band', None, 'patch')
The draws below stay inside these ranges and needn't reach their ends.
Inputs may be any that keep to these rules, and one draw needn't show every extreme that they name: `owners`: no patch owns more than 8 tiles, and one patch owns exactly 8.
All inputs are finite; a program needn't handle non-finite values.
Results may differ from the reference program's by a relative error of at most 0.003.
Values may be sent and summed in bfloat16 or wider, within the bound.
A program may use at most 64 MiB of HBM per device.

```python
import jax
import jax.numpy as jnp
from jax import lax

D = 512
BLK = 128
TILES = 16
MESH_DEV = 2560
CH = 12
CAP = 8
CELLS_T = 1024
MESH = 10240
BANDS = 8
N_PATCH = 4


def draw_owners(key, part):
    key_heavy, key_order, key_offset = jax.random.split(jax.random.fold_in(key, 11), 3)
    heavy_owner = jax.random.randint(key_heavy, (), 0, N_PATCH)
    tile_order = jax.random.permutation(key_order, TILES)
    offset_draw = jax.random.randint(key_offset, (), 0, N_PATCH - 1)
    position = jnp.arange(TILES)
    others = (heavy_owner + 1 + (position - CAP + offset_draw) % (N_PATCH - 1)) % N_PATCH
    owner_by_position = jnp.where(position < CAP, heavy_owner, others).astype(jnp.int32)
    return jnp.zeros((TILES,), jnp.int32).at[tile_order].set(owner_by_position)


def place_ends(drawn, own_key, smallest, high):
    extent = drawn.shape
    spot = [jax.random.randint(jax.random.fold_in(own_key, axis), (), 0, extent[axis]) for axis in range(len(extent))]
    drawn = drawn.at[tuple(spot)].set(smallest)
    longest = extent.index(max(extent))
    spot[longest] = (spot[longest] + 1) % extent[longest]
    return drawn.at[tuple(spot)].set(high)


def steps_of(own_key, shape, pieces, low, top_value):
    loudness = 1.0
    for axis_at, shards_of in pieces:
        steps = jax.random.uniform(jax.random.fold_in(jax.random.fold_in(own_key, 6), axis_at), (shards_of,), jnp.float32, low / len(pieces), top_value / len(pieces))
        loudness = loudness * jnp.repeat(jnp.exp(steps), shape[axis_at] // shards_of).reshape((-1,) + (1,) * (len(shape) - 1 - axis_at))
    return loudness


def noise(own_key, extent, spread, limit, pieces=(), kind=jnp.bfloat16):
    array = spread * jax.random.normal(own_key, extent, jnp.float32)
    if pieces:
        array = array * steps_of(own_key, extent, pieces, -0.22, 0.18)
    return jnp.clip(array, -limit, limit).astype(kind)


def setup_inputs(seed: int = 0) -> dict:
    keys = jax.random.split(jax.random.key(seed), 12)
    latents = noise(keys[0], (BANDS, MESH, D), 1.0, 6.0, ((0, 8), (1, 4)))
    owners = draw_owners(jax.random.fold_in(keys[11], 71), 0)
    block_rows = place_ends(jax.random.randint(keys[2], (TILES, BLK), 0, MESH_DEV), jax.random.fold_in(keys[2], 1), 0, MESH_DEV - 1).astype(jnp.int32)
    interp_weights = noise(keys[3], (TILES, CELLS_T, BLK), BLK ** -0.5, 0.5, ((0, 8), (1, 4)))
    w_first = noise(keys[4], (BANDS, D, D), D ** -0.5, 0.25, ((0, 8),))
    b_first = noise(keys[5], (BANDS, D), 0.5, 3.0, ((0, 8),), jnp.float32)
    w_second = noise(keys[6], (BANDS, D, D), D ** -0.5, 0.25, ((0, 8),))
    b_second = noise(keys[7], (BANDS, D), 1.0, 4.0, ((0, 8),), jnp.float32)
    gain = jnp.clip(1.0 + 0.18 * jax.random.normal(keys[8], (BANDS, D), jnp.float32), 0.1, 1.9)
    w_out = noise(keys[9], (BANDS, CH, D), D ** -0.5, 0.25, ((0, 8),))
    b_out = noise(keys[10], (BANDS, CH), 1.0, 4.0, ((0, 8),), jnp.float32)
    return {"latents": latents, "owners": owners, "block_rows": block_rows, "interp_weights": interp_weights, "w_first": w_first, "b_first": b_first, "w_second": w_second, "b_second": b_second, "gain": gain, "w_out": w_out, "b_out": b_out}


def decode_rows(interp, w_first, b_first, w_second, b_second, gain, w_out, b_out):
    hidden = jax.nn.silu(jnp.dot(interp, w_first, preferred_element_type=jnp.float32) + b_first).astype(jnp.bfloat16)
    second = jnp.dot(hidden, w_second, preferred_element_type=jnp.float32) + b_second
    mean_value = lax.optimization_barrier(jnp.mean(second, axis=-1, keepdims=True))
    centred = second - mean_value
    variance = lax.optimization_barrier(jnp.mean(centred * centred, axis=-1, keepdims=True))
    normed = (centred * lax.rsqrt(variance + 1e-05) * gain).astype(jnp.bfloat16)
    result = lax.dot_general(w_out, normed, (((1,), (1,)), ((), ())), preferred_element_type=jnp.float32)
    return result + b_out[:, None]

def reference(latents, owners, block_rows, interp_weights, w_first, b_first, w_second, b_second, gain, w_out, b_out):
    mesh_dev = latents.shape[1] // N_PATCH

    def one_band(band_args):
        band_latents, first_w, first_b, second_w, second_b, band_gain, out_w, out_b = band_args

        def one_tile(tile_index):
            rows_global = owners[tile_index] * mesh_dev + block_rows[tile_index]
            block = jnp.take(band_latents, rows_global.astype(jnp.int32), axis=0)
            interp = jnp.dot(interp_weights[tile_index], block, preferred_element_type=jnp.float32).astype(jnp.bfloat16)
            return decode_rows(interp, first_w, first_b, second_w, second_b, band_gain, out_w, out_b)
        per_tile = lax.map(one_tile, jnp.arange(TILES, dtype=jnp.int32))
        return jnp.transpose(per_tile, (1, 0, 2)).reshape(per_tile.shape[1], -1)
    return lax.map(one_band, (latents, w_first, b_first, w_second, b_second, gain, w_out, b_out))
```

```python
import functools

import jax
import jax.numpy as jnp
from jax import lax
from jax.experimental import pallas as pl
from jax.experimental.pallas import tpu as pltpu
from jax.sharding import PartitionSpec as P

EXT = 32
PARTS = 2


def contract_last(a, b):
    return lax.dot_general(a, b, (((1,), (1,)), ((), ())), preferred_element_type=jnp.float32)


def split(value):
    high = value.astype(jnp.bfloat16)
    return high, value - high.astype(jnp.float32)


def when(condition, action):
    if condition is True:
        action()
    elif condition is not False:
        pl.when(condition)(action)


def kernel(
    nb, np_, tiles, blk, cl, slots,
    owners, rows, w_b1, w_b2, w_gain, w_out, w_bo, latents, pieces, w_first, w_second,
    out,
    lat, w1, w2, mine, perm, onehot, own0, own1, sib0, sib1, far, from_chip, weights,
    w1t, w2e, b2b, bft, rank_of,
    lat_sem, wt_sem, mine_sem, piece_send, w_recv, z_send, x_send,
    sib_send, sib_recv, chip_send, chip_recv,
):
    b, p = lax.axis_index("band"), lax.axis_index("patch")
    n_chips = np_ // 2
    tb, tp = tiles // nb, tiles // np_
    g = tp // tb
    n_z = nb // 2
    q, c = p // 2, p % 2
    z, x = b // 2, b % 2
    mesh_dev, width = latents.shape
    wide = width // 2
    rows_u = 2 * cl
    channels = w_bo.shape[1]
    bf16, f32 = jnp.bfloat16, jnp.float32
    own, sib = (own0, own1), (sib0, sib1)

    def remote(src, dst, send, recv, band, patch):
        return pltpu.make_async_remote_copy(
            src_ref=src, dst_ref=dst, send_sem=send, recv_sem=recv,
            device_id={"band": band, "patch": patch}, device_id_type=pl.DeviceIdType.MESH,
        )

    home = b // g
    home_here = home // 2 == q
    own_source = b % g

    def source(jj):
        j = (x + jj) % g
        band = p * g + j
        on_line = jj % 2 == 0 if g % 2 == 0 else band % 2 == x
        return j, band // 2, on_line

    barrier = pltpu.get_barrier_semaphore()

    def greet(band, patch):
        pl.semaphore_signal(
            barrier, inc=1, device_id={"band": band, "patch": patch},
            device_id_type=pl.DeviceIdType.MESH,
        )

    greet(b, 2 * q + 1 - c)
    for d in range(1, n_chips):
        greet(b, 2 * ((q + d) % n_chips) + c)
    greet(2 * z + 1 - x, p)
    greet(2 * ((z + 1) % n_z) + x, p)
    for jj in range(g):
        _, zs, on_line = source(jj)
        if on_line is False:
            continue
        for e in range(np_):
            pp = (p + e) % np_
            sends = (pp // 2 == q) | ((z + zs) % 2 == 0)
            if e == 0:
                sends = sends & (zs != z)
            if on_line is not True:
                sends = sends & on_line
            when(sends, lambda zs=zs, pp=pp: greet(2 * zs + x, pp))
    greetings = n_chips + 2 + jnp.where(home_here, n_z - (home == p).astype(jnp.int32), n_z // 2)

    depth = mesh_dev // lat_sem.shape[0]
    lat_copies = [
        pltpu.make_async_copy(
            latents.at[pl.ds(k * depth, depth)], lat.at[pl.ds(k * depth, depth)], lat_sem.at[k]
        )
        for k in range(lat_sem.shape[0])
    ]
    mine_copies = [pltpu.make_async_copy(pieces.at[i], mine.at[i], mine_sem.at[i]) for i in range(tb)]
    for copy in mine_copies + lat_copies:
        copy.start()
    w1_copy = pltpu.make_async_copy(w_first, w1, wt_sem.at[0])
    w2_copy = pltpu.make_async_copy(w_second, w2, wt_sem.at[1])
    w1_copy.start()
    w2_copy.start()

    owner = [owners[t] for t in range(tiles)]
    rank = []
    for t in range(tiles):
        r = jnp.int32(0)
        for u in range(t):
            r = r + (owner[u] == owner[t]).astype(jnp.int32)
        rank.append(r)
        rank_of[t] = jnp.minimum(r, slots - 1)
    mark = [jnp.where(owner[t] == p, rank[t], -1) for t in range(tiles)]
    perm[...] = jnp.full(perm.shape, -1, jnp.int32)
    for s in range(slots):
        tile = jnp.int32(0)
        for t in range(tiles):
            tile = tile + jnp.where(mark[t] == s, t, 0)
        perm[s : s + 1, :] = rows[pl.ds(tile, 1), :]
    columns = perm[...].T
    iota = lax.broadcasted_iota(jnp.int32, (blk, mesh_dev), 1)
    for s in range(slots):
        hit = iota == columns[:, s : s + 1]
        onehot[s * blk : (s + 1) * blk, :] = jnp.where(hit, 1.0, 0.0).astype(bf16)

    pl.semaphore_wait(barrier, greetings)

    def piece_copy(i, dz):
        return remote(
            mine.at[i],
            weights.at[own_source * tb + i, pl.ds(pl.multiple_of(p * cl, cl), cl)],
            piece_send.at[i, dz], w_recv.at[own_source, i, p],
            2 * ((z + dz) % n_z) + x, home,
        )

    def piece_sends(dz):
        if dz == 0:
            return home != p
        return home_here if dz % 2 else True

    away = sorted(range(n_z), key=lambda dz: -min(dz, n_z - dz))
    for i in range(tb):
        mine_copies[i].wait()
        for dz in away:
            when(piece_sends(dz), lambda i=i, dz=dz: piece_copy(i, dz).start())

    @pl.when(home == p)
    def _():
        for i in range(tb):
            pltpu.make_async_copy(
                pieces.at[i],
                weights.at[own_source * tb + i, pl.ds(pl.multiple_of(p * cl, cl), cl)],
                w_recv.at[own_source, i, p],
            ).start()

    def chunk(j, i, at):
        part = weights.at[j * tb + i, pl.ds(pl.multiple_of(at * cl, cl), cl)]
        return part, w_recv.at[j, i, at]

    def arrive(j, i, at):
        part, recv = chunk(j, i, at)
        pltpu.make_async_copy(part, part, recv).wait()

    def along_z(j, i, at):
        part, recv = chunk(j, i, at)
        return remote(part, part, z_send.at[i, at], recv, 2 * ((z + n_z - 1) % n_z) + x, p)

    def along_x(j, i, at):
        part, recv = chunk(j, i, at)
        return remote(part, part, x_send.at[i, at], recv, 2 * z + 1 - x, p)

    def each_chunk(jj, i, dd, act):
        j, zs, on_line = source(jj)

        def body():
            for half in range(2):
                act(j, zs, i, dd, ((q + dd) % n_chips) * 2 + half)

        when(on_line, body)

    def relay_one(j, zs, i, dd, at):
        arrive(j, i, at)
        if dd:
            pl.when((z + zs) % 2 == 0)(lambda: along_z(j, i, at).start())
        along_x(j, i, at).start()

    def drain_one(j, zs, i, dd, at):
        if dd:
            pl.when((z + zs) % 2 == 0)(lambda: along_z(j, i, at).wait_send())
        along_x(j, i, at).wait_send()

    def relay(i, dd):
        for jj in range(g):
            each_chunk(jj, i, dd, relay_one)

    per = slots // PARTS

    def to_sibling(h, k):
        at = pl.ds(k * per, per)
        return remote(
            own[h].at[at], sib[h].at[at], sib_send.at[h, k], sib_recv.at[h, k], b, 2 * q + 1 - c
        )

    for copy in lat_copies:
        copy.wait()
    for h in range(2):
        for k in range(PARTS):
            part = jnp.dot(
                onehot[k * per * blk : (k + 1) * per * blk, :], lat[:, h * wide : (h + 1) * wide],
                preferred_element_type=f32,
            )
            own[h][k * per : (k + 1) * per] = part.astype(bf16).reshape(per, blk, wide)
            to_sibling(h, k).start()

    def tile_of(kk):
        return ((x + kk // tb) % g) * tb + kk % tb

    def from_this_chip(h, t):
        return jnp.where(owners[t] == p, own[h][rank_of[t]], sib[h][rank_of[t]])

    def to_chip(h, d, kk):
        return remote(
            far.at[h, d - 1, kk], from_chip.at[h, d - 1, kk],
            chip_send.at[h, d - 1, kk], chip_recv.at[h, d - 1, kk],
            b, 2 * ((q + d) % n_chips) + c,
        )

    def send_far(h):
        for k in range(PARTS):
            to_sibling(h, k).wait_recv()
        for kk in range(tp):
            for d in range(1, n_chips):
                t = (2 * ((q + d) % n_chips) + c) * tp + tile_of(kk)
                far[h, d - 1, kk] = from_this_chip(h, t)
                to_chip(h, d, kk).start()

    send_far(0)
    relay(0, 0)
    send_far(1)
    for i in range(tb):
        for dd in range(n_chips):
            if i or dd:
                relay(i, dd)

    w1_copy.wait()
    w2_copy.wait()
    eye = jnp.where(
        lax.broadcasted_iota(jnp.int32, (width, width), 0)
        == lax.broadcasted_iota(jnp.int32, (width, width), 1), 1.0, 0.0,
    ).astype(bf16)
    w1t[...] = (0.5 * contract_last(eye, w1[...])).astype(bf16)
    w2e[EXT:, :] = contract_last(eye, w2[...]).astype(bf16)
    pad = EXT // 2
    scaled = jnp.concatenate(
        [w_out[...].astype(f32) * w_gain[...], jnp.zeros((pad - channels, width), f32)], axis=0
    )
    high, rest = split(scaled)
    mid, rest = split(rest)
    ones = jnp.full((pad, width), 1.0 / width, f32).astype(bf16)
    sums = contract_last(jnp.concatenate([high, mid, rest.astype(bf16), ones], axis=0), w2[...])
    mean_row = sums[3 * pad : 3 * pad + 1]
    head = sums[:pad] + sums[pad : 2 * pad] + sums[2 * pad : 3 * pad]
    head = head - jnp.sum(scaled, axis=1, keepdims=True) * mean_row
    head = jnp.where(lax.broadcasted_iota(jnp.int32, head.shape, 0) == channels, mean_row, head)
    high, rest = split(head)
    w2e[:pad, :] = high
    w2e[pad:EXT, :] = rest.astype(bf16)
    b2c = w_b2[...] - jnp.mean(w_b2[...], axis=1, keepdims=True)
    head_bias = jnp.sum(scaled * b2c, axis=1, keepdims=True)
    b2b[...] = jnp.transpose(jnp.broadcast_to(b2c, (128, width)))
    high, rest = split(jnp.transpose(jnp.broadcast_to(0.5 * w_b1[...], (128, width))))
    mid, rest = split(rest)
    lane = lax.broadcasted_iota(jnp.int32, (width, 128), 1)
    terms = (high.astype(f32), mid.astype(f32), rest)
    bias_columns = jnp.zeros((width, 128), f32)
    for k, term in enumerate(terms):
        bias_columns = jnp.where(lane == k, term, bias_columns)
    bft[:, blk:] = bias_columns.astype(bf16)
    diagonal = lax.broadcasted_iota(jnp.int32, (pad, channels), 0) == lax.broadcasted_iota(
        jnp.int32, (pad, channels), 1
    )
    bias = jnp.sum(jnp.where(diagonal, w_bo[...], 0.0), axis=1, keepdims=True)
    ones_columns = jnp.where(
        lax.broadcasted_iota(jnp.int32, (rows_u, 128), 1) < len(terms), 1.0, 0.0
    ).astype(bf16)

    for kk in range(tp):
        jj, i = kk // tb, kk % tb
        j, _, on_line = source(jj)
        tile = tile_of(kk)
        t = p * tp + tile
        halves = []
        for h in range(2):
            value = from_this_chip(h, t)
            for d in range(1, n_chips):
                to_chip(h, d, kk).wait_recv()
                chip = 2 * ((q + n_chips - d) % n_chips)
                there = (owners[t] == chip) | (owners[t] == chip + 1)
                value = jnp.where(there, from_chip[h, d - 1, kk], value)
            halves.append(value)
        block = jnp.concatenate(halves, axis=1)
        bft[:, :blk] = contract_last(w1t[...], block).astype(bf16)

        for dd in range(n_chips):
            qq = (q + dd) % n_chips

            def rest_arrives():
                for half in range(2):
                    arrive(j, i, qq * 2 + half)

            if on_line is not True:
                when(True if on_line is False else jnp.logical_not(on_line), rest_arrives)
            start = pl.multiple_of(qq * rows_u, rows_u)
            cells = jnp.concatenate([weights[tile, pl.ds(start, rows_u), :], ones_columns], axis=1)
            half_v = contract_last(bft[...], cells)
            hidden = (half_v * jnp.tanh(half_v) + half_v).astype(bf16)
            second = jnp.dot(w2e[...], hidden, preferred_element_type=f32)
            heads = second[:pad] + second[pad:EXT]
            mean = heads[channels : channels + 1]
            centred = second[EXT:] + jnp.concatenate([b2b[...]] * (rows_u // 128), axis=1) - mean
            variance = jnp.sum(centred * centred, axis=0, keepdims=True) * (1.0 / width)
            result = (heads + head_bias) * lax.rsqrt(variance + 1e-05) + bias
            at = pl.multiple_of(tile * (np_ * cl) + start, rows_u)
            for ch in range(channels):
                out[ch, :, pl.ds(at, rows_u)] = result[ch : ch + 1]

    for i in range(tb):
        for dz in away:
            when(piece_sends(dz), lambda i=i, dz=dz: piece_copy(i, dz).wait_send())
    for h in range(2):
        for k in range(PARTS):
            to_sibling(h, k).wait_send()
        for d in range(1, n_chips):
            for kk in range(tp):
                to_chip(h, d, kk).wait_send()
    for jj in range(g):
        for i in range(tb):
            for dd in range(n_chips):
                each_chunk(jj, i, dd, drain_one)


def solution(mesh):
    nb, np_ = mesh.shape["band"], mesh.shape["patch"]

    def body(
        latents, owners, block_rows, pieces, w_first, b_first, w_second, b_second, gain, w_out, b_out
    ):
        tiles, blk = block_rows.shape
        cl, channels = pieces.shape[1], w_out.shape[1]
        mesh_dev, width = latents.shape[1:]
        n_chips, tb, tp = np_ // 2, tiles // nb, tiles // np_
        g = tp // tb
        n_z = nb // 2
        slots = tiles // 2
        far = max(n_chips - 1, 1)
        lat_parts = next(k for k in (5, 4, 2, 1) if mesh_dev % (k * 16) == 0)
        vmem = pl.BlockSpec(memory_space=pltpu.VMEM)
        hbm = pl.BlockSpec(memory_space=pl.ANY)
        bf16 = jnp.bfloat16
        dma = pltpu.SemaphoreType.DMA
        result = pl.pallas_call(
            functools.partial(kernel, nb, np_, tiles, blk, cl, slots),
            out_shape=jax.ShapeDtypeStruct((channels, 1, tp * np_ * cl), jnp.float32),
            in_specs=[pl.BlockSpec(memory_space=pltpu.SMEM)] + [vmem] * 6 + [hbm] * 4,
            out_specs=vmem,
            scratch_shapes=[
                pltpu.VMEM((mesh_dev, width), bf16),
                pltpu.VMEM(w_first.shape[1:], bf16),
                pltpu.VMEM(w_second.shape[1:], bf16),
                pltpu.VMEM((tb, cl, blk), bf16),
                pltpu.VMEM((blk, blk), jnp.int32),
                pltpu.VMEM((slots * blk, mesh_dev), bf16),
            ]
            + [pltpu.VMEM((slots, blk, width // 2), bf16)] * 4
            + [
                pltpu.VMEM((2, far, tp, blk, width // 2), bf16),
                pltpu.VMEM((2, far, tp, blk, width // 2), bf16),
                pltpu.VMEM((tp, np_ * cl, blk), bf16),
                pltpu.VMEM((width, width), bf16),
                pltpu.VMEM((EXT + width, width), bf16),
                pltpu.VMEM((width, 128), jnp.float32),
                pltpu.VMEM((width, blk + 128), bf16),
                pltpu.SMEM((tiles,), jnp.int32),
                dma((lat_parts,)),
                dma((2,)),
                dma((tb,)),
                dma((tb, n_z)),
                dma((g, tb, np_)),
                dma((tb, np_)),
                dma((tb, np_)),
                dma((2, PARTS)),
                dma((2, PARTS)),
                dma((2, far, tp)),
                dma((2, far, tp)),
            ],
            compiler_params=pltpu.CompilerParams(collective_id=0, has_side_effects=True),
            name="decode",
        )(
            owners, block_rows, b_first, b_second, gain, w_out[0], b_out,
            latents[0], pieces, w_first[0], w_second[0],
        )
        return jnp.transpose(result, (1, 0, 2))

    return jax.shard_map(
        body,
        mesh=mesh,
        in_specs=(
            P("band", "patch", None),
            P(),
            P(),
            P("band", "patch", None),
            P("band", None, None),
            P("band", None),
            P("band", None, None),
            P("band", None),
            P("band", None),
            P("band", None, None),
            P("band", None),
        ),
        out_specs=P("band", None, "patch"),
        check_vma=False,
    )
```

```python
import functools

import jax
import jax.numpy as jnp
from jax import lax
from jax.experimental import pallas as pl
from jax.experimental.pallas import tpu as pltpu
from jax.sharding import PartitionSpec as P

EXT = 32
PARTS = 2


def contract_last(a, b):
    return lax.dot_general(a, b, (((1,), (1,)), ((), ())), preferred_element_type=jnp.float32)


def split(value):
    high = value.astype(jnp.bfloat16)
    return high, value - high.astype(jnp.float32)


def when(condition, action):
    if condition is True:
        action()
    elif condition is not False:
        pl.when(condition)(action)


def kernel(
    nb, np_, tiles, blk, cl, slots,
    owners_in, rows_in, b1_in, b2_in, gain_in, out_in, bo_in, latents, pieces, w_first, w_second,
    out,
    owners, rows, w_b1, w_b2, w_gain, w_out, w_bo, lat, w1, w2, mine, perm, onehot, own0, own1, sib0, sib1, far, from_chip, weights,
    w1t, w2e, b2b, bft, fields, rank_of,
    small_sem, lat_sem, wt_sem, mine_sem, piece_send, w_recv, z_send, x_send,
    sib_send, sib_recv, chip_send, chip_recv, out_sem,
):
    b, p = lax.axis_index("band"), lax.axis_index("patch")
    n_chips = np_ // 2
    tb, tp = tiles // nb, tiles // np_
    g = tp // tb
    n_z = nb // 2
    q, c = p // 2, p % 2
    z, x = b // 2, b % 2
    mesh_dev, width = latents.shape
    wide = width // 2
    in_tile = np_ * cl
    channels = w_bo.shape[1]
    bf16, f32 = jnp.bfloat16, jnp.float32
    own, sib = (own0, own1), (sib0, sib1)

    def remote(src, dst, send, recv, band, patch):
        return pltpu.make_async_remote_copy(
            src_ref=src, dst_ref=dst, send_sem=send, recv_sem=recv,
            device_id={"band": band, "patch": patch}, device_id_type=pl.DeviceIdType.MESH,
        )

    home = b // g
    home_here = home // 2 == q
    own_source = b % g

    n_pair = n_z // 2
    pair = z + 1 - 2 * (z % 2)

    def seed(m):
        return 2 * ((z // 2 + m) % n_pair) + z % 2

    def source(jj):
        j = (x + jj) % g
        band = p * g + j
        on_line = jj % 2 == 0 if g % 2 == 0 else band % 2 == x
        return j, band // 2, on_line

    def place(zs):
        return jnp.where(
            z // 2 == zs // 2, jnp.where(z == zs, 0, 1), jnp.where(z % 2 == zs % 2, 2, 3)
        )

    barrier = pltpu.get_barrier_semaphore()

    def greet(band, patch):
        pl.semaphore_signal(
            barrier, inc=1, device_id={"band": band, "patch": patch},
            device_id_type=pl.DeviceIdType.MESH,
        )

    greet(b, 2 * q + 1 - c)
    for d in range(1, n_chips):
        greet(b, 2 * ((q + d) % n_chips) + c)
    greet(2 * z + 1 - x, p)
    greet(2 * pair + x, p)
    for m in range(1, n_pair):
        greet(2 * seed(m) + x, p)
    for jj in range(g):
        _, zs, on_line = source(jj)
        if on_line is False:
            continue
        at_line = place(zs)
        for e in range(np_):
            pp = (p + e) % np_
            across = (at_line == 0) | (at_line == 2) if tb > 1 else at_line == 0
            sends = jnp.where(pp // 2 == q, at_line != 3, across)
            if e == 0:
                sends = sends & (at_line != 0)
            if on_line is not True:
                sends = sends & on_line
            when(sends, lambda zs=zs, pp=pp: greet(2 * zs + x, pp))
    outgoing = n_pair + 1 - (home == p).astype(jnp.int32)
    greetings = n_chips + 1 + n_pair + jnp.where(home_here, outgoing, n_pair if tb > 1 else 1)

    depth = mesh_dev // lat_sem.shape[0]
    lat_copies = [
        pltpu.make_async_copy(
            latents.at[pl.ds(k * depth, depth)], lat.at[pl.ds(k * depth, depth)], lat_sem.at[k]
        )
        for k in range(lat_sem.shape[0])
    ]
    mine_copies = [pltpu.make_async_copy(pieces.at[i], mine.at[i], mine_sem.at[i]) for i in range(tb)]
    small = [
        pltpu.make_async_copy(src, dst, small_sem.at[k])
        for k, (src, dst) in enumerate((
            (owners_in, owners), (rows_in, rows), (b1_in, w_b1), (b2_in, w_b2),
            (gain_in, w_gain), (out_in, w_out), (bo_in, w_bo),
        ))
    ]
    for copy in small[:2] + lat_copies + mine_copies + small[2:]:
        copy.start()
    w1_copy = pltpu.make_async_copy(w_first, w1, wt_sem.at[0])
    w2_copy = pltpu.make_async_copy(w_second, w2, wt_sem.at[1])
    w1_copy.start()
    w2_copy.start()

    for copy in small[:2]:
        copy.wait()
    owner = [owners[t] for t in range(tiles)]
    rank = []
    for t in range(tiles):
        r = jnp.int32(0)
        for u in range(t):
            r = r + (owner[u] == owner[t]).astype(jnp.int32)
        rank.append(r)
        rank_of[t] = jnp.minimum(r, slots - 1)
    mark = [jnp.where(owner[t] == p, rank[t], -1) for t in range(tiles)]
    perm[...] = jnp.full(perm.shape, -1, jnp.int32)
    for s in range(slots):
        tile = jnp.int32(0)
        for t in range(tiles):
            tile = tile + jnp.where(mark[t] == s, t, 0)
        perm[s : s + 1, :] = rows[pl.ds(tile, 1), :]
    columns = perm[...].T
    def piece_copy(i, k):
        return remote(
            mine.at[i],
            weights.at[own_source * tb + i, pl.ds(pl.multiple_of(p * cl, cl), cl)],
            piece_send.at[i, k], w_recv.at[own_source, i, p],
            2 * (seed(k) if k < n_pair else pair) + x, home,
        )

    def piece_sends(i, k):
        if k == 0:
            return home != p
        if k == n_pair or i % 2 == 0:
            return home_here
        return True

    away = list(range(1, n_pair + 1)) + [0]

    def send_pieces():
        for i in range(tb):
            mine_copies[i].wait()
            for k in away:
                when(piece_sends(i, k), lambda i=i, k=k: piece_copy(i, k).start())

        @pl.when(home == p)
        def _():
            for i in range(tb):
                pltpu.make_async_copy(
                    pieces.at[i],
                    weights.at[own_source * tb + i, pl.ds(pl.multiple_of(p * cl, cl), cl)],
                    w_recv.at[own_source, i, p],
                ).start()

    def chunk(j, i, at):
        part = weights.at[j * tb + i, pl.ds(pl.multiple_of(at * cl, cl), cl)]
        return part, w_recv.at[j, i, at]

    def arrive(j, i, at):
        part, recv = chunk(j, i, at)
        pltpu.make_async_copy(part, part, recv).wait()

    def along_z(j, i, at, k):
        part, recv = chunk(j, i, at)
        return remote(part, part, z_send.at[k, i, at], recv, 2 * (seed(k) if k else pair) + x, p)

    def along_x(j, i, at):
        part, recv = chunk(j, i, at)
        return remote(part, part, x_send.at[i, at], recv, 2 * z + 1 - x, p)

    def onward(at_line, j, i, dd, at):
        copies = []
        if at_line == 2 or (at_line == 0 and dd):
            copies.append(along_z(j, i, at, 0))
        if at_line == 0 and dd and i % 2 == 0:
            copies += [along_z(j, i, at, m) for m in range(1, n_pair)]
        return copies + [along_x(j, i, at)]

    def relay(at_line, chunks, act="relay"):
        for jj in range(g):
            j, zs, on_line = source(jj)
            if on_line is False:
                continue

            def body(j=j):
                for i, dd in chunks:
                    for half in range(2):
                        at = ((q + dd) % n_chips) * 2 + half
                        if act == "relay":
                            arrive(j, i, at)
                        for copy in onward(at_line, j, i, dd, at):
                            if act == "relay":
                                copy.start()
                            else:
                                copy.wait_send()

            here = place(zs) == at_line
            when(here if on_line is True else here & on_line, body)

    per = slots // PARTS

    def to_sibling(h, k):
        at = pl.ds(k * per, per)
        return remote(
            own[h].at[at], sib[h].at[at], sib_send.at[h, k], sib_recv.at[h, k], b, 2 * q + 1 - c
        )

    def gather(h):
        done = [
            jnp.dot(
                onehot[k * per * blk : (k + 1) * per * blk, :], lat[:, h * wide : (h + 1) * wide],
                preferred_element_type=f32,
            )
            for k in range(PARTS)
        ]
        for k in range(PARTS):
            own[h][k * per : (k + 1) * per] = done[k].astype(bf16).reshape(per, blk, wide)

    def front(send):
        iota = lax.broadcasted_iota(jnp.int32, (blk, mesh_dev), 1)
        for s in range(slots):
            hit = iota == columns[:, s : s + 1]
            onehot[s * blk : (s + 1) * blk, :] = jnp.where(hit, 1.0, 0.0).astype(bf16)
        for copy in lat_copies:
            copy.wait()
        for h in range(2):
            gather(h)
            if send:
                for k in range(PARTS):
                    to_sibling(h, k).start()

    pl.when(z == 0)(lambda: front(False))
    pl.semaphore_wait(barrier, greetings)
    send_pieces()

    @pl.when(z == 0)
    def _():
        for h in range(2):
            for k in range(PARTS):
                to_sibling(h, k).start()

    pl.when(z != 0)(lambda: front(True))

    def tile_of(kk):
        return ((x + kk // tb) % g) * tb + kk % tb

    def from_this_chip(h, t):
        return jnp.where(owners[t] == p, own[h][rank_of[t]], sib[h][rank_of[t]])

    def to_chip(h, d, kk):
        return remote(
            far.at[h, d - 1, kk], from_chip.at[h, d - 1, kk],
            chip_send.at[h, d - 1, kk], chip_recv.at[h, d - 1, kk],
            b, 2 * ((q + d) % n_chips) + c,
        )

    def send_far(h, kk):
        for d in range(1, n_chips):
            t = (2 * ((q + d) % n_chips) + c) * tp + tile_of(kk)
            far[h, d - 1, kk] = from_this_chip(h, t)
            to_chip(h, d, kk).start()

    def sibling_here(h):
        for k in range(PARTS):
            to_sibling(h, k).wait_recv()

    sibling_here(0)
    first = max(tp // 2, 1)
    for kk in range(first):
        send_far(0, kk)
    every = [(i, 0) for i in range(tb)]
    across = [(i, dd) for i in range(tb) for dd in range(1, n_chips)]
    back = [(i, dd) for i in reversed(range(tb)) for dd in range(1, n_chips)]
    early = {0: every + across[: n_chips - 1], 1: every[:1], 2: every[:1], 3: []}
    late = {0: across[n_chips - 1 :], 1: every[1:] + across, 2: every[1:] + back, 3: every + back}
    for k in range(4):
        relay(k, early[k])
    for copy in small[2:]:
        copy.wait()
    w1_copy.wait()
    w2_copy.wait()
    eye = jnp.where(
        lax.broadcasted_iota(jnp.int32, (width, width), 0)
        == lax.broadcasted_iota(jnp.int32, (width, width), 1), 1.0, 0.0,
    ).astype(bf16)
    w1t[...] = (0.5 * contract_last(eye, w1[...])).astype(bf16)
    w2e[EXT:, :] = contract_last(eye, w2[...]).astype(bf16)
    pad = EXT // 2
    scaled = jnp.concatenate(
        [w_out[...].astype(f32) * w_gain[...], jnp.zeros((pad - channels, width), f32)], axis=0
    )
    high, rest = split(scaled)
    mid, rest = split(rest)
    ones = jnp.full((pad, width), 1.0 / width, f32).astype(bf16)
    sums = contract_last(jnp.concatenate([high, mid, rest.astype(bf16), ones], axis=0), w2[...])
    mean_row = sums[3 * pad : 3 * pad + 1]
    head = sums[:pad] + sums[pad : 2 * pad] + sums[2 * pad : 3 * pad]
    head = head - jnp.sum(scaled, axis=1, keepdims=True) * mean_row
    head = jnp.where(lax.broadcasted_iota(jnp.int32, head.shape, 0) == channels, mean_row, head)
    high, rest = split(head)
    w2e[:pad, :] = high
    w2e[pad:EXT, :] = rest.astype(bf16)
    b2c = w_b2[...] - jnp.mean(w_b2[...], axis=1, keepdims=True)
    head_bias = jnp.sum(scaled * b2c, axis=1, keepdims=True)
    b2b[...] = jnp.transpose(jnp.broadcast_to(b2c, (128, width)))
    high, rest = split(jnp.transpose(jnp.broadcast_to(0.5 * w_b1[...], (128, width))))
    mid, rest = split(rest)
    lane = lax.broadcasted_iota(jnp.int32, (width, 128), 1)
    terms = (high.astype(f32), mid.astype(f32), rest)
    bias_columns = jnp.zeros((width, 128), f32)
    for k, term in enumerate(terms):
        bias_columns = jnp.where(lane == k, term, bias_columns)
    bft[:, blk:] = bias_columns.astype(bf16)
    diagonal = lax.broadcasted_iota(jnp.int32, (pad, channels), 0) == lax.broadcasted_iota(
        jnp.int32, (pad, channels), 1
    )
    bias = jnp.sum(jnp.where(diagonal, w_bo[...], 0.0), axis=1, keepdims=True)
    ones_columns = jnp.where(
        lax.broadcasted_iota(jnp.int32, (in_tile, 128), 1) < len(terms), 1.0, 0.0
    ).astype(bf16)

    sibling_here(1)
    for kk in range(first):
        send_far(1, kk)
    for kk in range(first, tp):
        for h in range(2):
            send_far(h, kk)
    for k in range(4):
        relay(k, late[k])

    def out_copy(kk, tile):
        cells = pl.ds(pl.multiple_of(tile * in_tile, in_tile), in_tile)
        return pltpu.make_async_copy(
            fields.at[:, :, cells], out.at[:, :, cells], out_sem.at[kk]
        )

    for kk in range(tp):
        jj, i = kk // tb, kk % tb
        j, _, on_line = source(jj)
        tile = tile_of(kk)
        t = p * tp + tile
        halves = []
        for h in range(2):
            value = from_this_chip(h, t)
            for d in range(1, n_chips):
                to_chip(h, d, kk).wait_recv()
                chip = 2 * ((q + n_chips - d) % n_chips)
                there = (owners[t] == chip) | (owners[t] == chip + 1)
                value = jnp.where(there, from_chip[h, d - 1, kk], value)
            halves.append(value)
        block = jnp.concatenate(halves, axis=1)

        def rest_arrives(j=j, i=i):
            for at in range(np_):
                arrive(j, i, at)

        if on_line is not True:
            when(True if on_line is False else jnp.logical_not(on_line), rest_arrives)
        for r in range(2):
            at = slice(r * wide, (r + 1) * wide)
            bft[at, :blk] = contract_last(w1t[at, :], block).astype(bf16)
        cells = jnp.concatenate([weights[tile], ones_columns], axis=1)
        half_v = contract_last(bft[...], cells)
        hidden = (half_v * jnp.tanh(half_v) + half_v).astype(bf16)
        second = jnp.dot(w2e[...], hidden, preferred_element_type=f32)
        heads = second[:pad] + second[pad:EXT]
        mean = heads[channels : channels + 1]
        centred = second[EXT:] + jnp.concatenate([b2b[...]] * (in_tile // 128), axis=1) - mean
        variance = jnp.sum(centred * centred, axis=0, keepdims=True) * (1.0 / width)
        result = (heads + head_bias) * lax.rsqrt(variance + 1e-05) + bias
        at = pl.multiple_of(tile * in_tile, in_tile)
        for ch in range(channels):
            fields[ch, :, pl.ds(at, in_tile)] = result[ch : ch + 1]
        out_copy(kk, tile).start()

    for i in range(tb):
        for k in away:
            when(piece_sends(i, k), lambda i=i, k=k: piece_copy(i, k).wait_send())
    for h in range(2):
        for k in range(PARTS):
            to_sibling(h, k).wait_send()
        for d in range(1, n_chips):
            for kk in range(tp):
                to_chip(h, d, kk).wait_send()
    for k in range(4):
        relay(k, every + across, "drain")
    for kk in range(tp):
        out_copy(kk, tile_of(kk)).wait()


def solution(mesh):
    nb, np_ = mesh.shape["band"], mesh.shape["patch"]

    def body(
        latents, owners, block_rows, pieces, w_first, b_first, w_second, b_second, gain, w_out, b_out
    ):
        tiles, blk = block_rows.shape
        cl, channels = pieces.shape[1], w_out.shape[1]
        mesh_dev, width = latents.shape[1:]
        n_chips, tb, tp = np_ // 2, tiles // nb, tiles // np_
        g = tp // tb
        n_z = nb // 2
        slots = tiles // 2
        far = max(n_chips - 1, 1)
        lat_parts = next(k for k in (5, 4, 2, 1) if mesh_dev % (k * 16) == 0)
        hbm = pl.BlockSpec(memory_space=pltpu.HBM)
        bf16 = jnp.bfloat16
        dma = pltpu.SemaphoreType.DMA
        result = pl.pallas_call(
            functools.partial(kernel, nb, np_, tiles, blk, cl, slots),
            out_shape=jax.ShapeDtypeStruct((channels, 1, tp * np_ * cl), jnp.float32),
            in_specs=[hbm] * 11,
            out_specs=hbm,
            scratch_shapes=[
                pltpu.SMEM((tiles,), jnp.int32),
                pltpu.VMEM((tiles, blk), jnp.int32),
                pltpu.VMEM((1, width), jnp.float32),
                pltpu.VMEM((1, width), jnp.float32),
                pltpu.VMEM((1, width), jnp.float32),
                pltpu.VMEM((channels, width), bf16),
                pltpu.VMEM((1, channels), jnp.float32),
                pltpu.VMEM((mesh_dev, width), bf16),
                pltpu.VMEM(w_first.shape[1:], bf16),
                pltpu.VMEM(w_second.shape[1:], bf16),
                pltpu.VMEM((tb, cl, blk), bf16),
                pltpu.VMEM((blk, blk), jnp.int32),
                pltpu.VMEM((slots * blk, mesh_dev), bf16),
            ]
            + [pltpu.VMEM((slots, blk, width // 2), bf16)] * 4
            + [
                pltpu.VMEM((2, far, tp, blk, width // 2), bf16),
                pltpu.VMEM((2, far, tp, blk, width // 2), bf16),
                pltpu.VMEM((tp, np_ * cl, blk), bf16),
                pltpu.VMEM((width, width), bf16),
                pltpu.VMEM((EXT + width, width), bf16),
                pltpu.VMEM((width, 128), jnp.float32),
                pltpu.VMEM((width, blk + 128), bf16),
                pltpu.VMEM((channels, 1, tp * np_ * cl), jnp.float32),
                pltpu.SMEM((tiles,), jnp.int32),
                dma((7,)),
                dma((lat_parts,)),
                dma((2,)),
                dma((tb,)),
                dma((tb, n_z // 2 + 1)),
                dma((g, tb, np_)),
                dma((n_z // 2, tb, np_)),
                dma((tb, np_)),
                dma((2, PARTS)),
                dma((2, PARTS)),
                dma((2, far, tp)),
                dma((2, far, tp)),
                dma((tp,)),
            ],
            compiler_params=pltpu.CompilerParams(collective_id=0, has_side_effects=True),
            name="decode",
        )(
            owners, block_rows, b_first, b_second, gain, w_out[0], b_out,
            latents[0], pieces, w_first[0], w_second[0],
        )
        return jnp.transpose(result, (1, 0, 2))

    return jax.shard_map(
        body,
        mesh=mesh,
        in_specs=(
            P("band", "patch", None),
            P(),
            P(),
            P("band", "patch", None),
            P("band", None, None),
            P("band", None),
            P("band", None, None),
            P("band", None),
            P("band", None),
            P("band", None, None),
            P("band", None),
        ),
        out_specs=P("band", None, "patch"),
        check_vma=False,
    )
```

```python
import functools

import jax
import jax.numpy as jnp
from jax import lax
from jax.experimental import pallas as pl
from jax.experimental.pallas import tpu as pltpu
from jax.sharding import PartitionSpec as P

EXT = 32
PARTS = 2


def contract_last(a, b):
    return lax.dot_general(a, b, (((1,), (1,)), ((), ())), preferred_element_type=jnp.float32)


def split(value):
    high = value.astype(jnp.bfloat16)
    return high, value - high.astype(jnp.float32)


def when(condition, action):
    if condition is True:
        action()
    elif condition is not False:
        pl.when(condition)(action)


def kernel(
    nb, np_, tiles, blk, cl, slots,
    owners_in, rows_in, b1_in, b2_in, gain_in, out_in, bo_in, latents, pieces, w_first, w_second,
    out,
    owners, rows, w_rows, w_out, w_bo, lat, w_both, mine, perm, onehot, own0, own1, sib0, sib1, far, from_chip, weights,
    w1t, w2e, b2b, bft, fields, rank_of,
    small_sem, lat_sem, wt_sem, mine_sem, piece_send, w_recv, z_send, x_send,
    sib_send, sib_recv, chip_send, chip_recv, out_sem,
):
    b, p = lax.axis_index("band"), lax.axis_index("patch")
    n_chips = np_ // 2
    tb, tp = tiles // nb, tiles // np_
    g = tp // tb
    n_z = nb // 2
    q, c = p // 2, p % 2
    z, x = b // 2, b % 2
    mesh_dev, width = latents.shape
    wide = width // 2
    in_tile = np_ * cl
    channels = w_bo.shape[1]
    bf16, f32 = jnp.bfloat16, jnp.float32
    own, sib = (own0, own1), (sib0, sib1)

    def remote(src, dst, send, recv, band, patch):
        return pltpu.make_async_remote_copy(
            src_ref=src, dst_ref=dst, send_sem=send, recv_sem=recv,
            device_id={"band": band, "patch": patch}, device_id_type=pl.DeviceIdType.MESH,
        )

    home = b // g
    home_here = home // 2 == q
    own_source = b % g

    n_pair = n_z // 2
    pair = z + 1 - 2 * (z % 2)

    def seed(m):
        return 2 * ((z // 2 + m) % n_pair) + z % 2

    def source(jj):
        j = (x + jj) % g
        band = p * g + j
        on_line = jj % 2 == 0 if g % 2 == 0 else band % 2 == x
        return j, band // 2, on_line

    def place(zs):
        return jnp.where(
            z // 2 == zs // 2, jnp.where(z == zs, 0, 1), jnp.where(z % 2 == zs % 2, 2, 3)
        )

    barrier = pltpu.get_barrier_semaphore()

    def greet(band, patch):
        pl.semaphore_signal(
            barrier, inc=1, device_id={"band": band, "patch": patch},
            device_id_type=pl.DeviceIdType.MESH,
        )

    greet(b, 2 * q + 1 - c)
    for d in range(1, n_chips):
        greet(b, 2 * ((q + d) % n_chips) + c)
    greet(2 * z + 1 - x, p)
    greet(2 * pair + x, p)
    for m in range(1, n_pair):
        greet(2 * seed(m) + x, p)
    for jj in range(g):
        _, zs, on_line = source(jj)
        at_line = place(zs)
        for e in range(np_):
            pp = (p + e) % np_
            if on_line is not False:
                sends = (at_line % 2 == 0) | ((pp // 2 == q) & (at_line == 1))
                if e == 0:
                    sends = sends & (at_line != 0)
                if on_line is not True:
                    sends = sends & on_line
                when(sends, lambda zs=zs, pp=pp: greet(2 * zs + x, pp))
            if on_line is not True:
                sends = (pp // 2 == q) & (at_line == 0)
                if on_line is not False:
                    sends = sends & jnp.logical_not(on_line)
                when(sends, lambda zs=zs, pp=pp: greet(2 * zs + 1 - x, pp))
    outgoing = n_pair + 2 - (home == p).astype(jnp.int32)
    greetings = n_chips + 1 + n_pair + jnp.where(home_here, outgoing, n_pair)

    lat_copy = pltpu.make_async_copy(latents, lat, lat_sem.at[0])
    mine_copy = pltpu.make_async_copy(pieces, mine, mine_sem.at[0])
    small = [
        pltpu.make_async_copy(src, dst, small_sem.at[k])
        for k, (src, dst) in enumerate((
            (owners_in, owners), (rows_in, rows), (out_in, w_out), (bo_in, w_bo),
        ))
    ]
    rows_of_width = [
        pltpu.make_async_copy(src, w_rows.at[k], small_sem.at[4])
        for k, src in enumerate((b1_in, b2_in, gain_in))
    ]
    wide_copies = [
        pltpu.make_async_copy(src, w_both.at[k], wt_sem.at[0]) for k, src in enumerate((w_first, w_second))
    ]
    for copy in small[:2] + [lat_copy, mine_copy] + small[2:] + rows_of_width + wide_copies:
        copy.start()

    for copy in small[:2]:
        copy.wait()
    owner = [owners[t] for t in range(tiles)]
    rank = []
    for t in range(tiles):
        r = jnp.int32(0)
        for u in range(t):
            r = r + (owner[u] == owner[t]).astype(jnp.int32)
        rank.append(r)
        rank_of[t] = jnp.minimum(r, slots - 1)
    mark = [jnp.where(owner[t] == p, rank[t], -1) for t in range(tiles)]
    perm[...] = jnp.full(perm.shape, -1, jnp.int32)
    for s in range(slots):
        tile = jnp.int32(0)
        for t in range(tiles):
            tile = tile + jnp.where(mark[t] == s, t, 0)
        perm[s : s + 1, :] = rows[pl.ds(tile, 1), :]
    columns = perm[...].T
    def piece_copy(i, k):
        return remote(
            mine.at[i],
            weights.at[own_source * tb + i, pl.ds(pl.multiple_of(p * cl, cl), cl)],
            piece_send.at[k], w_recv.at[own_source, i, p],
            2 * z + 1 - x if k > n_pair else 2 * (seed(k) if k < n_pair else pair) + x, home,
        )

    def piece_sends(k):
        if k == 0:
            return home != p
        return home_here if k >= n_pair else True

    away = list(range(1, n_pair)) + [n_pair + 1, 0, n_pair]

    def send_pieces():
        mine_copy.wait()
        for k in away:
            for i in range(tb) if k == 0 else reversed(range(tb)):
                when(piece_sends(k), lambda i=i, k=k: piece_copy(i, k).start())

        @pl.when(home == p)
        def _():
            for i in range(tb):
                pltpu.make_async_copy(
                    pieces.at[i],
                    weights.at[own_source * tb + i, pl.ds(pl.multiple_of(p * cl, cl), cl)],
                    w_recv.at[own_source, i, p],
                ).start()

    def chunk(j, i, at):
        part = weights.at[j * tb + i, pl.ds(pl.multiple_of(at * cl, cl), cl)]
        return part, w_recv.at[j, i, at]

    def arrive(j, i, at):
        part, recv = chunk(j, i, at)
        pltpu.make_async_copy(part, part, recv).wait()

    def along_z(j, i, at, k, other=0):
        part, recv = chunk(j, i, at)
        return remote(
            part, part, z_send.at[(k or n_pair) if other else 0], recv, 2 * (seed(k) if k else pair) + x, p
        )

    def along_x(j, i, at):
        part, recv = chunk(j, i, at)
        return remote(part, part, x_send.at[0], recv, 2 * z + 1 - x, p)

    def crosses_early(i, dd):
        return dd > 0 and i % 2 == 0

    def onward(at_line, j, i, dd, at):
        copies = []
        if at_line == 2 or (at_line == 0 and dd):
            copies.append(along_z(j, i, at, 0))
        if (at_line == 0 and dd) or at_line == 1 or (at_line > 1 and not crosses_early(i, dd)):
            copies.append(along_x(j, i, at))
        return copies

    def onward_other(at_line, j, i, at):
        if at_line == 0:
            return [along_z(j, i, at, m, 1) for m in range(1, n_pair)]
        return [along_z(j, i, at, 0, 1)]

    def relay(at_line, chunks, other=False):
        for jj in range(g):
            j, zs, on_line = source(jj)
            if on_line is other:
                continue

            def body(j=j):
                for i, dd in chunks:
                    for half in range(2):
                        at = ((q + dd) % n_chips) * 2 + half
                        arrive(j, i, at)
                        if other:
                            copies = onward_other(at_line, j, i, at)
                        else:
                            copies = onward(at_line, j, i, dd, at)
                        for copy in copies:
                            copy.start()

            here = place(zs) == at_line
            if on_line is not True and on_line is not False:
                here = here & (jnp.logical_not(on_line) if other else on_line)
            if chunks:
                when(here, body)

    def sent(sem, count):
        if count:
            a = next(a for a in range(1, tp + 1) if count % a == 0 and count // a <= np_)
            part = weights.at[pl.ds(0, a), pl.ds(0, count // a * cl)]
            remote(part, part, sem, w_recv.at[0, 0, 0], 2 * z + 1 - x, p).wait_send()

    def relay_drain(at_line):
        across = [(i, dd) for i in range(tb) for dd in range(1, n_chips)]
        even = [1 for i, dd in across if crosses_early(i, dd)]
        in_plane, over, early = 2 * tb, 2 * len(across), 2 * len(even)
        along = {0: over, 1: 0, 2: in_plane + over, 3: 0}[at_line]
        beside = {0: over, 1: in_plane + over, 2: in_plane + over - early, 3: in_plane + over - early}[at_line]
        for jj in range(g):
            _, zs, on_line = source(jj)
            here = place(zs) == at_line

            def body():
                sent(z_send.at[0], along)
                sent(x_send.at[0], beside)

            def body_other():
                for m in range(1, n_pair) if at_line == 0 else (n_pair,):
                    sent(z_send.at[m], early)

            if on_line is not False:
                when(here if on_line is True else here & on_line, body)
            if on_line is not True and at_line % 2 == 0:
                when(here if on_line is False else here & jnp.logical_not(on_line), body_other)

    per = slots // PARTS

    def to_sibling(h):
        return remote(own[h], sib[h], sib_send.at[h], sib_recv.at[h], b, 2 * q + 1 - c)

    def gather(h):
        done = [
            jnp.dot(
                onehot[k * per * blk : (k + 1) * per * blk, :], lat[:, h * wide : (h + 1) * wide],
                preferred_element_type=f32,
            )
            for k in range(PARTS)
        ]
        for k in range(PARTS):
            own[h][k * per : (k + 1) * per] = done[k].astype(bf16).reshape(per, blk, wide)

    def share(h):
        to_sibling(h).start()

    def front(h):
        if h == 0:
            lat_copy.wait()
        gather(h)

    def build():
        iota = lax.broadcasted_iota(jnp.int32, (blk, mesh_dev), 1)
        for s in range(slots):
            hit = iota == columns[:, s : s + 1]
            onehot[s * blk : (s + 1) * blk, :] = jnp.where(hit, 1.0, 0.0).astype(bf16)

    pl.when(z < n_pair)(build)
    pl.when(z == 0)(lambda: front(0))
    pl.semaphore_wait(barrier, greetings)
    pl.when(z == 0)(lambda: share(0))
    send_pieces()
    pl.when(z >= n_pair)(build)

    @pl.when(z != 0)
    def _():
        front(0)
        share(0)

    front(1)
    share(1)

    def step_of(kk):
        return kk // tb, tb - 1 - kk % tb

    def tile_of(kk):
        jj, i = step_of(kk)
        return ((x + jj) % g) * tb + i

    def from_this_chip(h, t):
        return jnp.where(owners[t] == p, own[h][rank_of[t]], sib[h][rank_of[t]])

    def to_chip(h, d, kk):
        return remote(
            far.at[d - 1, kk, h], from_chip.at[d - 1, kk, h], chip_send.at[0], chip_recv.at[d - 1, kk],
            b, 2 * ((q + d) % n_chips) + c,
        )

    def chip_here(d, kk):
        part = from_chip.at[d - 1, kk]
        pltpu.make_async_copy(part, part, chip_recv.at[d - 1, kk]).wait()

    def send_far(h, kk):
        for d in range(1, n_chips):
            t = (2 * ((q + d) % n_chips) + c) * tp + tile_of(kk)
            far[d - 1, kk, h] = from_this_chip(h, t)
            to_chip(h, d, kk).start()

    def sibling_here(h):
        to_sibling(h).wait_recv()

    sibling_here(0)
    first = max(tp // 2, 1)
    for kk in range(first):
        send_far(0, kk)
    every = [(i, 0) for i in reversed(range(tb))]
    even = [(i, dd) for i in range(0, tb, 2) for dd in range(1, n_chips)]
    odd = [(i, dd) for i in range(1, tb, 2) for dd in range(1, n_chips)]
    early = {0: even, 2: every[:1]}
    late = {0: odd + every, 1: every[:1] + odd + every[1:], 2: odd + every[1:] + even, 3: every[:1] + odd}
    last = {1: even, 3: every[1:] + even}

    @pl.when(z != 0)
    def _():
        for k in early:
            relay(k, early[k])

    for copy in small[2:]:
        copy.wait()
    pltpu.make_async_copy(w_rows, w_rows, small_sem.at[4]).wait()
    pltpu.make_async_copy(w_both, w_both, wt_sem.at[0]).wait()
    w1, w2 = w_both.at[0], w_both.at[1]
    w_b1, w_b2, w_gain = (w_rows.at[k] for k in range(3))
    eye = jnp.where(
        lax.broadcasted_iota(jnp.int32, (width, width), 0)
        == lax.broadcasted_iota(jnp.int32, (width, width), 1), 1.0, 0.0,
    ).astype(bf16)
    w1t[...] = (0.5 * contract_last(eye, w1[...])).astype(bf16)
    w2e[EXT:, :] = contract_last(eye, w2[...]).astype(bf16)
    pad = EXT // 2
    scaled = jnp.concatenate(
        [w_out[...].astype(f32) * w_gain[...], jnp.zeros((pad - channels, width), f32)], axis=0
    )
    high, rest = split(scaled)
    mid, rest = split(rest)
    ones = jnp.full((pad, width), 1.0 / width, f32).astype(bf16)
    sums = contract_last(jnp.concatenate([high, mid, rest.astype(bf16), ones], axis=0), w2[...])
    mean_row = sums[3 * pad : 3 * pad + 1]
    head = sums[:pad] + sums[pad : 2 * pad] + sums[2 * pad : 3 * pad]
    head = head - jnp.sum(scaled, axis=1, keepdims=True) * mean_row
    head = jnp.where(lax.broadcasted_iota(jnp.int32, head.shape, 0) == channels, mean_row, head)
    high, rest = split(head)
    w2e[:pad, :] = high
    w2e[pad:EXT, :] = rest.astype(bf16)
    b2c = w_b2[...] - jnp.mean(w_b2[...], axis=1, keepdims=True)
    head_bias = jnp.sum(scaled * b2c, axis=1, keepdims=True)
    b2b[...] = jnp.transpose(jnp.broadcast_to(b2c, (128, width)))
    high, rest = split(jnp.transpose(jnp.broadcast_to(0.5 * w_b1[...], (128, width))))
    mid, rest = split(rest)
    lane = lax.broadcasted_iota(jnp.int32, (width, 128), 1)
    terms = (high.astype(f32), mid.astype(f32), rest)
    bias_columns = jnp.zeros((width, 128), f32)
    for k, term in enumerate(terms):
        bias_columns = jnp.where(lane == k, term, bias_columns)
    bft[:, blk:] = bias_columns.astype(bf16)
    diagonal = lax.broadcasted_iota(jnp.int32, (pad, channels), 0) == lax.broadcasted_iota(
        jnp.int32, (pad, channels), 1
    )
    bias = jnp.sum(jnp.where(diagonal, w_bo[...], 0.0), axis=1, keepdims=True)
    ones_columns = jnp.where(
        lax.broadcasted_iota(jnp.int32, (in_tile, 128), 1) < len(terms), 1.0, 0.0
    ).astype(bf16)

    sibling_here(1)
    for kk in range(first):
        send_far(1, kk)
    for kk in range(first, tp):
        for h in range(2):
            send_far(h, kk)
    @pl.when(z == 0)
    def _():
        for k in early:
            relay(k, early[k])

    for k in late:
        relay(k, late[k])
    pl.when(z != 0)(lambda: relay(0, even, other=True))

    def out_copy(kk, tile):
        cells = pl.ds(pl.multiple_of(tile * in_tile, in_tile), in_tile)
        return pltpu.make_async_copy(
            fields.at[:, :, cells], out.at[:, :, cells], out_sem.at[0]
        )

    for kk in range(tp):
        jj, i = step_of(kk)
        j, zs, on_line = source(jj)
        if kk == min(1, tb - 1):
            for k in last:
                relay(k, last[k])
            pl.when(z == 0)(lambda: relay(0, even, other=True))
            relay(2, even, other=True)
        tile = tile_of(kk)
        t = p * tp + tile
        for d in range(1, n_chips):
            chip_here(d, kk)
        halves = []
        for h in range(2):
            value = from_this_chip(h, t)
            for d in range(1, n_chips):
                chip = 2 * ((q + n_chips - d) % n_chips)
                there = (owners[t] == chip) | (owners[t] == chip + 1)
                value = jnp.where(there, from_chip[d - 1, kk, h], value)
            halves.append(value)
        block = jnp.concatenate(halves, axis=1)

        def rest_arrives(j=j, i=i, zs=zs):
            for dd in range(n_chips):

                def wait(dd=dd):
                    for half in range(2):
                        arrive(j, i, ((q + dd) % n_chips) * 2 + half)

                when(place(zs) % 2 == 1 if crosses_early(i, dd) else True, wait)

        if on_line is not True:
            when(True if on_line is False else jnp.logical_not(on_line), rest_arrives)
        for r in range(2):
            at = slice(r * wide, (r + 1) * wide)
            bft[at, :blk] = contract_last(w1t[at, :], block).astype(bf16)
        cells = jnp.concatenate([weights[tile], ones_columns], axis=1)
        half_v = contract_last(bft[...], cells)
        hidden = (half_v * jnp.tanh(half_v) + half_v).astype(bf16)
        second = jnp.dot(w2e[...], hidden, preferred_element_type=f32)
        heads = second[:pad] + second[pad:EXT]
        mean = heads[channels : channels + 1]
        centred = second[EXT:] + jnp.concatenate([b2b[...]] * (in_tile // 128), axis=1) - mean
        variance = jnp.sum(centred * centred, axis=0, keepdims=True) * (1.0 / width)
        result = (heads + head_bias) * lax.rsqrt(variance + 1e-05) + bias
        at = pl.multiple_of(tile * in_tile, in_tile)
        for ch in range(channels):
            fields[ch, :, pl.ds(at, in_tile)] = result[ch : ch + 1]
        out_copy(kk, tile).start()

    def pieces_sent(k):
        return remote(mine, mine, piece_send.at[k], w_recv.at[0, 0, 0], 2 * z + 1 - x, home)

    for k in away:
        when(piece_sends(k), lambda k=k: pieces_sent(k).wait_send())
    for h in range(2):
        to_sibling(h).wait_send()
    if n_chips > 1:
        remote(far, far, chip_send.at[0], chip_recv.at[0, 0], b, 2 * q + 1 - c).wait_send()
    for k in range(4):
        relay_drain(k)
    pltpu.make_async_copy(fields, out, out_sem.at[0]).wait()


def solution(mesh):
    nb, np_ = mesh.shape["band"], mesh.shape["patch"]

    def body(
        latents, owners, block_rows, pieces, w_first, b_first, w_second, b_second, gain, w_out, b_out
    ):
        tiles, blk = block_rows.shape
        cl, channels = pieces.shape[1], w_out.shape[1]
        mesh_dev, width = latents.shape[1:]
        n_chips, tb, tp = np_ // 2, tiles // nb, tiles // np_
        g = tp // tb
        n_z = nb // 2
        slots = tiles // 2
        far = max(n_chips - 1, 1)
        hbm = pl.BlockSpec(memory_space=pltpu.HBM)
        bf16 = jnp.bfloat16
        dma = pltpu.SemaphoreType.DMA
        result = pl.pallas_call(
            functools.partial(kernel, nb, np_, tiles, blk, cl, slots),
            out_shape=jax.ShapeDtypeStruct((channels, 1, tp * np_ * cl), jnp.float32),
            in_specs=[hbm] * 11,
            out_specs=hbm,
            scratch_shapes=[
                pltpu.SMEM((tiles,), jnp.int32),
                pltpu.VMEM((tiles, blk), jnp.int32),
                pltpu.VMEM((3, 1, width), jnp.float32),
                pltpu.VMEM((channels, width), bf16),
                pltpu.VMEM((1, channels), jnp.float32),
                pltpu.VMEM((mesh_dev, width), bf16),
                pltpu.VMEM((2,) + w_first.shape[1:], bf16),
                pltpu.VMEM((tb, cl, blk), bf16),
                pltpu.VMEM((blk, blk), jnp.int32),
                pltpu.VMEM((slots * blk, mesh_dev), bf16),
            ]
            + [pltpu.VMEM((slots, blk, width // 2), bf16)] * 4
            + [
                pltpu.VMEM((far, tp, 2, blk, width // 2), bf16),
                pltpu.VMEM((far, tp, 2, blk, width // 2), bf16),
                pltpu.VMEM((tp, np_ * cl, blk), bf16),
                pltpu.VMEM((width, width), bf16),
                pltpu.VMEM((EXT + width, width), bf16),
                pltpu.VMEM((width, 128), jnp.float32),
                pltpu.VMEM((width, blk + 128), bf16),
                pltpu.VMEM((channels, 1, tp * np_ * cl), jnp.float32),
                pltpu.SMEM((tiles,), jnp.int32),
                dma((5,)),
                dma((1,)),
                dma((1,)),
                dma((1,)),
                dma((n_z // 2 + 2,)),
                dma((g, tb, np_)),
                dma((n_z // 2 + 1,)),
                dma((1,)),
                dma((2,)),
                dma((2,)),
                dma((1,)),
                dma((far, tp)),
                dma((1,)),
            ],
            compiler_params=pltpu.CompilerParams(collective_id=0, has_side_effects=True),
            name="decode",
        )(
            owners, block_rows, b_first, b_second, gain, w_out[0], b_out,
            latents[0], pieces, w_first[0], w_second[0],
        )
        return jnp.transpose(result, (1, 0, 2))

    return jax.shard_map(
        body,
        mesh=mesh,
        in_specs=(
            P("band", "patch", None),
            P(),
            P(),
            P("band", "patch", None),
            P("band", None, None),
            P("band", None),
            P("band", None, None),
            P("band", None),
            P("band", None),
            P("band", None, None),
            P("band", None),
        ),
        out_specs=P("band", None, "patch"),
        check_vma=False,
    )
```

```python
import functools

import jax
import jax.numpy as jnp
from jax import lax
from jax.experimental import pallas as pl
from jax.experimental.pallas import tpu as pltpu
from jax.sharding import PartitionSpec as P

EXT = 32
PARTS = 2


def contract_last(a, b):
    return lax.dot_general(a, b, (((1,), (1,)), ((), ())), preferred_element_type=jnp.float32)


def split(value):
    high = value.astype(jnp.bfloat16)
    return high, value - high.astype(jnp.float32)


def when(condition, action):
    if condition is True:
        action()
    elif condition is not False:
        pl.when(condition)(action)


def kernel(
    nb, np_, tiles, blk, cl, slots,
    owners_in, rows_in, b1_in, b2_in, gain_in, out_in, bo_in, latents, pieces, w_first, w_second,
    out,
    owners, rows, w_rows, w_out, w_bo, lat, w_both, mine, perm, onehot, own0, own1, sib0, sib1, far, from_chip, weights,
    w1t, w2e, b2b, bft, rank_of,
    small_sem, lat_sem, wt_sem, mine_sem, piece_send, w_recv, z_send, x_send,
    sib_send, sib_recv, chip_send, chip_recv,
):
    b, p = lax.axis_index("band"), lax.axis_index("patch")
    n_chips = np_ // 2
    tb, tp = tiles // nb, tiles // np_
    g = tp // tb
    n_z = nb // 2
    q, c = p // 2, p % 2
    z, x = b // 2, b % 2
    mesh_dev, width = latents.shape
    wide = width // 2
    in_tile = np_ * cl
    channels = w_bo.shape[1]
    bf16, f32 = jnp.bfloat16, jnp.float32
    own, sib = (own0, own1), (sib0, sib1)

    def remote(src, dst, send, recv, band, patch):
        return pltpu.make_async_remote_copy(
            src_ref=src, dst_ref=dst, send_sem=send, recv_sem=recv,
            device_id={"band": band, "patch": patch}, device_id_type=pl.DeviceIdType.MESH,
        )

    home = b // g
    home_here = home // 2 == q
    own_source = b % g

    n_pair = n_z // 2
    pair = z + 1 - 2 * (z % 2)

    def seed(m):
        return 2 * ((z // 2 + m) % n_pair) + z % 2

    def source(jj):
        j = (x + jj) % g
        band = p * g + j
        on_line = jj % 2 == 0 if g % 2 == 0 else band % 2 == x
        return j, band // 2, on_line

    def place(zs):
        return jnp.where(
            z // 2 == zs // 2, jnp.where(z == zs, 0, 1), jnp.where(z % 2 == zs % 2, 2, 3)
        )

    barrier = pltpu.get_barrier_semaphore()

    def greet(band, patch):
        pl.semaphore_signal(
            barrier, inc=1, device_id={"band": band, "patch": patch},
            device_id_type=pl.DeviceIdType.MESH,
        )

    greet(b, 2 * q + 1 - c)
    for d in range(1, n_chips):
        greet(b, 2 * ((q + d) % n_chips) + c)
    greet(2 * z + 1 - x, p)
    greet(2 * pair + x, p)
    for m in range(1, n_pair):
        greet(2 * seed(m) + x, p)
    for jj in range(g):
        _, zs, on_line = source(jj)
        at_line = place(zs)
        for e in range(np_):
            pp = (p + e) % np_
            if on_line is not False:
                sends = (at_line % 2 == 0) | ((pp // 2 == q) & (at_line == 1))
                if e == 0:
                    sends = sends & (at_line != 0)
                if on_line is not True:
                    sends = sends & on_line
                when(sends, lambda zs=zs, pp=pp: greet(2 * zs + x, pp))
            if on_line is not True:
                sends = (pp // 2 == q) & (at_line == 0)
                if on_line is not False:
                    sends = sends & jnp.logical_not(on_line)
                when(sends, lambda zs=zs, pp=pp: greet(2 * zs + 1 - x, pp))
    outgoing = n_pair + 2 - (home == p).astype(jnp.int32)
    greetings = n_chips + 1 + n_pair + jnp.where(home_here, outgoing, n_pair)

    lat_copy = pltpu.make_async_copy(latents, lat, lat_sem.at[0])
    mine_copy = pltpu.make_async_copy(pieces, mine, mine_sem.at[0])
    small = [
        pltpu.make_async_copy(src, dst, small_sem.at[k])
        for k, (src, dst) in enumerate((
            (owners_in, owners), (rows_in, rows), (out_in, w_out), (bo_in, w_bo),
        ))
    ]
    rows_of_width = [
        pltpu.make_async_copy(src, w_rows.at[k], small_sem.at[4])
        for k, src in enumerate((b1_in, b2_in, gain_in))
    ]
    wide_copies = [
        pltpu.make_async_copy(src, w_both.at[k], wt_sem.at[0]) for k, src in enumerate((w_first, w_second))
    ]
    for copy in small[:2] + [lat_copy, mine_copy] + small[2:] + rows_of_width + wide_copies:
        copy.start()

    for copy in small[:2]:
        copy.wait()
    owner = [owners[t] for t in range(tiles)]
    rank = []
    for t in range(tiles):
        r = jnp.int32(0)
        for u in range(t):
            r = r + (owner[u] == owner[t]).astype(jnp.int32)
        rank.append(r)
        rank_of[t] = jnp.minimum(r, slots - 1)
    mark = [jnp.where(owner[t] == p, rank[t], -1) for t in range(tiles)]
    perm[...] = jnp.full(perm.shape, -1, jnp.int32)
    for s in range(slots):
        tile = jnp.int32(0)
        for t in range(tiles):
            tile = tile + jnp.where(mark[t] == s, t, 0)
        perm[s : s + 1, :] = rows[pl.ds(tile, 1), :]
    columns = perm[...].T
    def piece_copy(i, k):
        return remote(
            mine.at[i],
            weights.at[own_source * tb + i, pl.ds(pl.multiple_of(p * cl, cl), cl)],
            piece_send.at[k], w_recv.at[own_source, i, p],
            2 * z + 1 - x if k > n_pair else 2 * (seed(k) if k < n_pair else pair) + x, home,
        )

    def piece_sends(k):
        if k == 0:
            return home != p
        return home_here if k >= n_pair else True

    away = list(range(1, n_pair)) + [n_pair + 1, 0, n_pair]

    def send_pieces():
        mine_copy.wait()
        for k in away:
            for i in range(tb) if k == 0 else reversed(range(tb)):
                when(piece_sends(k), lambda i=i, k=k: piece_copy(i, k).start())

        @pl.when(home == p)
        def _():
            for i in range(tb):
                pltpu.make_async_copy(
                    pieces.at[i],
                    weights.at[own_source * tb + i, pl.ds(pl.multiple_of(p * cl, cl), cl)],
                    w_recv.at[own_source, i, p],
                ).start()

    def chunk(j, i, at):
        part = weights.at[j * tb + i, pl.ds(pl.multiple_of(at * cl, cl), cl)]
        return part, w_recv.at[j, i, at]

    def arrive(j, i, at):
        part, recv = chunk(j, i, at)
        pltpu.make_async_copy(part, part, recv).wait()

    def along_z(j, i, at, k, other=0):
        part, recv = chunk(j, i, at)
        return remote(
            part, part, z_send.at[(k or n_pair) if other else 0], recv, 2 * (seed(k) if k else pair) + x, p
        )

    def along_x(j, i, at):
        part, recv = chunk(j, i, at)
        return remote(part, part, x_send.at[0], recv, 2 * z + 1 - x, p)

    def crosses_early(i, dd):
        return dd > 0 and i % 2 == 0

    def onward(at_line, j, i, dd, at):
        copies = []
        if at_line == 2 or (at_line == 0 and dd):
            copies.append(along_z(j, i, at, 0))
        if (at_line == 0 and dd) or at_line == 1 or (at_line > 1 and not crosses_early(i, dd)):
            copies.append(along_x(j, i, at))
        return copies

    def onward_other(at_line, j, i, at):
        if at_line == 0:
            return [along_z(j, i, at, m, 1) for m in range(1, n_pair)]
        return [along_z(j, i, at, 0, 1)]

    def relay(at_line, chunks, other=False):
        for jj in range(g):
            j, zs, on_line = source(jj)
            if on_line is other:
                continue

            def body(j=j):
                for i, dd in chunks:
                    for half in range(2):
                        at = ((q + dd) % n_chips) * 2 + half
                        arrive(j, i, at)
                        if other:
                            copies = onward_other(at_line, j, i, at)
                        else:
                            copies = onward(at_line, j, i, dd, at)
                        for copy in copies:
                            copy.start()

            here = place(zs) == at_line
            if on_line is not True and on_line is not False:
                here = here & (jnp.logical_not(on_line) if other else on_line)
            if chunks:
                when(here, body)

    def sent(sem, count):
        if count:
            a = next(a for a in range(1, tp + 1) if count % a == 0 and count // a <= np_)
            part = weights.at[pl.ds(0, a), pl.ds(0, count // a * cl)]
            remote(part, part, sem, w_recv.at[0, 0, 0], 2 * z + 1 - x, p).wait_send()

    def relay_drain(at_line):
        across = [(i, dd) for i in range(tb) for dd in range(1, n_chips)]
        even = [1 for i, dd in across if crosses_early(i, dd)]
        in_plane, over, early = 2 * tb, 2 * len(across), 2 * len(even)
        along = {0: over, 1: 0, 2: in_plane + over, 3: 0}[at_line]
        beside = {0: over, 1: in_plane + over, 2: in_plane + over - early, 3: in_plane + over - early}[at_line]
        for jj in range(g):
            _, zs, on_line = source(jj)
            here = place(zs) == at_line

            def body():
                sent(z_send.at[0], along)
                sent(x_send.at[0], beside)

            def body_other():
                for m in range(1, n_pair) if at_line == 0 else (n_pair,):
                    sent(z_send.at[m], early)

            if on_line is not False:
                when(here if on_line is True else here & on_line, body)
            if on_line is not True and at_line % 2 == 0:
                when(here if on_line is False else here & jnp.logical_not(on_line), body_other)

    per = slots // PARTS

    def to_sibling(h):
        return remote(own[h], sib[h], sib_send.at[h], sib_recv.at[h], b, 2 * q + 1 - c)

    def gather(h):
        done = [
            jnp.dot(
                onehot[k * per * blk : (k + 1) * per * blk, :], lat[:, h * wide : (h + 1) * wide],
                preferred_element_type=f32,
            )
            for k in range(PARTS)
        ]
        for k in range(PARTS):
            own[h][k * per : (k + 1) * per] = done[k].astype(bf16).reshape(per, blk, wide)

    def share(h):
        to_sibling(h).start()

    def front(h):
        if h == 0:
            lat_copy.wait()
        gather(h)

    def build():
        iota = lax.broadcasted_iota(jnp.int32, (blk, mesh_dev), 1)
        for s in range(slots):
            hit = iota == columns[:, s : s + 1]
            onehot[s * blk : (s + 1) * blk, :] = jnp.where(hit, 1.0, 0.0).astype(bf16)

    pl.when(z < n_pair)(build)
    pl.when(z == 0)(lambda: front(0))
    pl.semaphore_wait(barrier, greetings)
    pl.when(z == 0)(lambda: share(0))
    send_pieces()
    pl.when(z >= n_pair)(build)

    @pl.when(z != 0)
    def _():
        front(0)
        share(0)

    front(1)
    share(1)

    def step_of(kk):
        return kk // tb, tb - 1 - kk % tb

    def tile_of(kk):
        jj, i = step_of(kk)
        return ((x + jj) % g) * tb + i

    def from_this_chip(h, t):
        return jnp.where(owners[t] == p, own[h][rank_of[t]], sib[h][rank_of[t]])

    def to_chip(h, d, kk):
        return remote(
            far.at[d - 1, kk, h], from_chip.at[d - 1, kk, h], chip_send.at[0], chip_recv.at[d - 1, kk],
            b, 2 * ((q + d) % n_chips) + c,
        )

    def chip_here(d, kk):
        part = from_chip.at[d - 1, kk]
        pltpu.make_async_copy(part, part, chip_recv.at[d - 1, kk]).wait()

    def send_far(h, kk):
        for d in range(1, n_chips):
            t = (2 * ((q + d) % n_chips) + c) * tp + tile_of(kk)
            far[d - 1, kk, h] = from_this_chip(h, t)
            to_chip(h, d, kk).start()

    def sibling_here(h):
        to_sibling(h).wait_recv()

    sibling_here(0)
    first = max(tp // 2, 1)
    for kk in range(first):
        send_far(0, kk)
    every = [(i, 0) for i in reversed(range(tb))]
    even = [(i, dd) for i in range(0, tb, 2) for dd in range(1, n_chips)]
    odd = [(i, dd) for i in range(1, tb, 2) for dd in range(1, n_chips)]
    early = {0: even, 2: every[:1]}
    late = {0: odd + every, 1: every[:1] + odd + every[1:], 2: odd + every[1:] + even, 3: every[:1] + odd}
    last = {1: even, 3: every[1:] + even}

    @pl.when(z != 0)
    def _():
        for k in early:
            relay(k, early[k])

    for copy in small[2:]:
        copy.wait()
    pltpu.make_async_copy(w_rows, w_rows, small_sem.at[4]).wait()
    pltpu.make_async_copy(w_both, w_both, wt_sem.at[0]).wait()
    w1, w2 = w_both.at[0], w_both.at[1]
    w_b1, w_b2, w_gain = (w_rows.at[k] for k in range(3))
    eye = jnp.where(
        lax.broadcasted_iota(jnp.int32, (width, width), 0)
        == lax.broadcasted_iota(jnp.int32, (width, width), 1), 1.0, 0.0,
    ).astype(bf16)
    w1t[...] = (0.5 * contract_last(eye, w1[...])).astype(bf16)
    w2e[EXT:, :] = contract_last(eye, w2[...]).astype(bf16)
    pad = EXT // 2
    scaled = jnp.concatenate(
        [w_out[...].astype(f32) * w_gain[...], jnp.zeros((pad - channels, width), f32)], axis=0
    )
    high, rest = split(scaled)
    mid, rest = split(rest)
    ones = jnp.full((pad, width), 1.0 / width, f32).astype(bf16)
    sums = contract_last(jnp.concatenate([high, mid, rest.astype(bf16), ones], axis=0), w2[...])
    mean_row = sums[3 * pad : 3 * pad + 1]
    head = sums[:pad] + sums[pad : 2 * pad] + sums[2 * pad : 3 * pad]
    head = head - jnp.sum(scaled, axis=1, keepdims=True) * mean_row
    head = jnp.where(lax.broadcasted_iota(jnp.int32, head.shape, 0) == channels, mean_row, head)
    high, rest = split(head)
    w2e[:pad, :] = high
    w2e[pad:EXT, :] = rest.astype(bf16)
    b2c = w_b2[...] - jnp.mean(w_b2[...], axis=1, keepdims=True)
    head_bias = jnp.sum(scaled * b2c, axis=1, keepdims=True)
    b2b[...] = jnp.transpose(jnp.broadcast_to(b2c, (128, width)))
    high, rest = split(jnp.transpose(jnp.broadcast_to(0.5 * w_b1[...], (128, width))))
    mid, rest = split(rest)
    lane = lax.broadcasted_iota(jnp.int32, (width, 128), 1)
    terms = (high.astype(f32), mid.astype(f32), rest)
    bias_columns = jnp.zeros((width, 128), f32)
    for k, term in enumerate(terms):
        bias_columns = jnp.where(lane == k, term, bias_columns)
    bft[:, blk:] = bias_columns.astype(bf16)
    diagonal = lax.broadcasted_iota(jnp.int32, (pad, channels), 0) == lax.broadcasted_iota(
        jnp.int32, (pad, channels), 1
    )
    bias = jnp.sum(jnp.where(diagonal, w_bo[...], 0.0), axis=1, keepdims=True)
    ones_columns = jnp.where(
        lax.broadcasted_iota(jnp.int32, (in_tile, 128), 1) < len(terms), 1.0, 0.0
    ).astype(bf16)

    sibling_here(1)
    for kk in range(first):
        send_far(1, kk)
    for kk in range(first, tp):
        for h in range(2):
            send_far(h, kk)
    @pl.when(z == 0)
    def _():
        for k in early:
            relay(k, early[k])

    for k in late:
        relay(k, late[k])
    pl.when(z != 0)(lambda: relay(0, even, other=True))

    for kk in range(tp):
        jj, i = step_of(kk)
        j, zs, on_line = source(jj)
        if kk == min(1, tb - 1):
            for k in last:
                relay(k, last[k])
            pl.when(z == 0)(lambda: relay(0, even, other=True))
            relay(2, even, other=True)
        tile = tile_of(kk)
        t = p * tp + tile
        for d in range(1, n_chips):
            chip_here(d, kk)
        halves = []
        for h in range(2):
            value = from_this_chip(h, t)
            for d in range(1, n_chips):
                chip = 2 * ((q + n_chips - d) % n_chips)
                there = (owners[t] == chip) | (owners[t] == chip + 1)
                value = jnp.where(there, from_chip[d - 1, kk, h], value)
            halves.append(value)
        block = jnp.concatenate(halves, axis=1)

        def rest_arrives(j=j, i=i, zs=zs):
            for dd in range(n_chips):

                def wait(dd=dd):
                    for half in range(2):
                        arrive(j, i, ((q + dd) % n_chips) * 2 + half)

                when(place(zs) % 2 == 1 if crosses_early(i, dd) else True, wait)

        if on_line is not True:
            when(True if on_line is False else jnp.logical_not(on_line), rest_arrives)
        for r in range(2):
            at = slice(r * wide, (r + 1) * wide)
            bft[at, :blk] = contract_last(w1t[at, :], block).astype(bf16)
        cells = jnp.concatenate([weights[tile], ones_columns], axis=1)
        half_v = contract_last(bft[...], cells)
        hidden = (half_v * jnp.tanh(half_v) + half_v).astype(bf16)
        second = jnp.dot(w2e[...], hidden, preferred_element_type=f32)
        heads = second[:pad] + second[pad:EXT]
        mean = heads[channels : channels + 1]
        centred = second[EXT:] + jnp.concatenate([b2b[...]] * (in_tile // 128), axis=1) - mean
        variance = jnp.sum(centred * centred, axis=0, keepdims=True) * (1.0 / width)
        result = (heads + head_bias) * lax.rsqrt(variance + 1e-05) + bias
        at = pl.multiple_of(tile * in_tile, in_tile)
        for ch in range(channels):
            out[ch, :, pl.ds(at, in_tile)] = result[ch : ch + 1]

    def pieces_sent(k):
        return remote(mine, mine, piece_send.at[k], w_recv.at[0, 0, 0], 2 * z + 1 - x, home)

    for k in away:
        when(piece_sends(k), lambda k=k: pieces_sent(k).wait_send())
    for h in range(2):
        to_sibling(h).wait_send()
    if n_chips > 1:
        remote(far, far, chip_send.at[0], chip_recv.at[0, 0], b, 2 * q + 1 - c).wait_send()
    for k in range(4):
        relay_drain(k)


def solution(mesh):
    nb, np_ = mesh.shape["band"], mesh.shape["patch"]

    def body(
        latents, owners, block_rows, pieces, w_first, b_first, w_second, b_second, gain, w_out, b_out
    ):
        tiles, blk = block_rows.shape
        cl, channels = pieces.shape[1], w_out.shape[1]
        mesh_dev, width = latents.shape[1:]
        n_chips, tb, tp = np_ // 2, tiles // nb, tiles // np_
        g = tp // tb
        n_z = nb // 2
        slots = tiles // 2
        far = max(n_chips - 1, 1)
        hbm = pl.BlockSpec(memory_space=pltpu.HBM)
        bf16 = jnp.bfloat16
        dma = pltpu.SemaphoreType.DMA
        result = pl.pallas_call(
            functools.partial(kernel, nb, np_, tiles, blk, cl, slots),
            out_shape=pltpu.VMEM((channels, 1, tp * np_ * cl), jnp.float32),
            in_specs=[hbm] * 11,
            out_specs=pl.BlockSpec(memory_space=pltpu.VMEM),
            scratch_shapes=[
                pltpu.SMEM((tiles,), jnp.int32),
                pltpu.VMEM((tiles, blk), jnp.int32),
                pltpu.VMEM((3, 1, width), jnp.float32),
                pltpu.VMEM((channels, width), bf16),
                pltpu.VMEM((1, channels), jnp.float32),
                pltpu.VMEM((mesh_dev, width), bf16),
                pltpu.VMEM((2,) + w_first.shape[1:], bf16),
                pltpu.VMEM((tb, cl, blk), bf16),
                pltpu.VMEM((blk, blk), jnp.int32),
                pltpu.VMEM((slots * blk, mesh_dev), bf16),
            ]
            + [pltpu.VMEM((slots, blk, width // 2), bf16)] * 4
            + [
                pltpu.VMEM((far, tp, 2, blk, width // 2), bf16),
                pltpu.VMEM((far, tp, 2, blk, width // 2), bf16),
                pltpu.VMEM((tp, np_ * cl, blk), bf16),
                pltpu.VMEM((width, width), bf16),
                pltpu.VMEM((EXT + width, width), bf16),
                pltpu.VMEM((width, 128), jnp.float32),
                pltpu.VMEM((width, blk + 128), bf16),
                pltpu.SMEM((tiles,), jnp.int32),
                dma((5,)),
                dma((1,)),
                dma((1,)),
                dma((1,)),
                dma((n_z // 2 + 2,)),
                dma((g, tb, np_)),
                dma((n_z // 2 + 1,)),
                dma((1,)),
                dma((2,)),
                dma((2,)),
                dma((1,)),
                dma((far, tp)),
            ],
            compiler_params=pltpu.CompilerParams(collective_id=0, has_side_effects=True),
            name="decode",
        )(
            owners, block_rows, b_first, b_second, gain, w_out[0], b_out,
            latents[0], pieces, w_first[0], w_second[0],
        )
        return jnp.transpose(result, (1, 0, 2))

    return jax.shard_map(
        body,
        mesh=mesh,
        in_specs=(
            P("band", "patch", None),
            P(),
            P(),
            P("band", "patch", None),
            P("band", None, None),
            P("band", None),
            P("band", None, None),
            P("band", None),
            P("band", None),
            P("band", None, None),
            P("band", None),
        ),
        out_specs=P("band", None, "patch"),
        check_vma=False,
    )
```

```python
import functools

import jax
import jax.numpy as jnp
from jax import lax
from jax.experimental import pallas as pl
from jax.experimental.pallas import tpu as pltpu
from jax.sharding import PartitionSpec as P

EXT = 32
PARTS = 2


def contract_last(a, b):
    return lax.dot_general(a, b, (((1,), (1,)), ((), ())), preferred_element_type=jnp.float32)


def split(value):
    high = value.astype(jnp.bfloat16)
    return high, value - high.astype(jnp.float32)


def when(condition, action):
    if condition is True:
        action()
    elif condition is not False:
        pl.when(condition)(action)


def kernel(
    nb, np_, tiles, blk, cl, slots,
    owners_in, rows_in, b1_in, b2_in, gain_in, out_in, bo_in, latents, pieces, w_first, w_second,
    out,
    owners, rows, w_rows, w_out, w_bo, lat, w_both, mine, perm, onehot, own0, own1, sib0, sib1, far, from_chip, weights,
    w1t, w2e, b2b, bft, rank_of,
    small_sem, lat_sem, wt_sem, mine_sem, piece_send, w_recv, z_send, x_send,
    sib_send, sib_recv, chip_send, chip_recv,
):
    b, p = lax.axis_index("band"), lax.axis_index("patch")
    n_chips = np_ // 2
    tb, tp = tiles // nb, tiles // np_
    g = tp // tb
    n_z = nb // 2
    q, c = p // 2, p % 2
    z, x = b // 2, b % 2
    mesh_dev, width = latents.shape
    wide = width // 2
    in_tile = np_ * cl
    channels = w_bo.shape[1]
    bf16, f32 = jnp.bfloat16, jnp.float32
    own, sib = (own0, own1), (sib0, sib1)

    def remote(src, dst, send, recv, band, patch):
        return pltpu.make_async_remote_copy(
            src_ref=src, dst_ref=dst, send_sem=send, recv_sem=recv,
            device_id={"band": band, "patch": patch}, device_id_type=pl.DeviceIdType.MESH,
        )

    home = b // g
    home_here = home // 2 == q
    own_source = b % g

    n_pair = n_z // 2
    pair = z + 1 - 2 * (z % 2)

    def seed(m):
        return 2 * ((z // 2 + m) % n_pair) + z % 2

    def source(jj):
        j = (x + jj) % g
        band = p * g + j
        on_line = jj % 2 == 0 if g % 2 == 0 else band % 2 == x
        return j, band // 2, on_line

    def place(zs):
        return jnp.where(
            z // 2 == zs // 2, jnp.where(z == zs, 0, 1), jnp.where(z % 2 == zs % 2, 2, 3)
        )

    barrier = pltpu.get_barrier_semaphore()

    def greet(band, patch):
        pl.semaphore_signal(
            barrier, inc=1, device_id={"band": band, "patch": patch},
            device_id_type=pl.DeviceIdType.MESH,
        )

    greet(b, 2 * q + 1 - c)
    for d in range(1, n_chips):
        greet(b, 2 * ((q + d) % n_chips) + c)
    greet(2 * z + 1 - x, p)
    greet(2 * pair + x, p)
    for m in range(1, n_pair):
        greet(2 * seed(m) + x, p)
    for jj in range(g):
        _, zs, on_line = source(jj)
        at_line = place(zs)
        for e in range(np_):
            pp = (p + e) % np_
            if on_line is not False:
                sends = (at_line % 2 == 0) | ((pp // 2 == q) & (at_line == 1))
                if e == 0:
                    sends = sends & (at_line != 0)
                if on_line is not True:
                    sends = sends & on_line
                when(sends, lambda zs=zs, pp=pp: greet(2 * zs + x, pp))
            if on_line is not True:
                sends = (pp // 2 == q) & (at_line == 0)
                if on_line is not False:
                    sends = sends & jnp.logical_not(on_line)
                when(sends, lambda zs=zs, pp=pp: greet(2 * zs + 1 - x, pp))
    outgoing = n_pair + 2 - (home == p).astype(jnp.int32)
    greetings = n_chips + 1 + n_pair + jnp.where(home_here, outgoing, n_pair)

    lat_copy = pltpu.make_async_copy(latents, lat, lat_sem.at[0])
    mine_copy = pltpu.make_async_copy(pieces, mine, mine_sem.at[0])
    small = [
        pltpu.make_async_copy(src, dst, small_sem.at[k])
        for k, (src, dst) in enumerate((
            (owners_in, owners), (rows_in, rows), (out_in, w_out), (bo_in, w_bo),
        ))
    ]
    rows_of_width = [
        pltpu.make_async_copy(src, w_rows.at[k], small_sem.at[4])
        for k, src in enumerate((b1_in, b2_in, gain_in))
    ]
    wide_copies = [
        pltpu.make_async_copy(src, w_both.at[k], wt_sem.at[0]) for k, src in enumerate((w_first, w_second))
    ]
    for copy in small[:2] + [lat_copy, mine_copy] + small[2:] + rows_of_width + wide_copies:
        copy.start()

    for copy in small[:2]:
        copy.wait()
    owner = [owners[t] for t in range(tiles)]
    rank = []
    for t in range(tiles):
        r = jnp.int32(0)
        for u in range(t):
            r = r + (owner[u] == owner[t]).astype(jnp.int32)
        rank.append(r)
        rank_of[t] = jnp.minimum(r, slots - 1)
    mark = [jnp.where(owner[t] == p, rank[t], -1) for t in range(tiles)]
    perm[...] = jnp.full(perm.shape, -1, jnp.int32)
    for s in range(slots):
        tile = jnp.int32(0)
        for t in range(tiles):
            tile = tile + jnp.where(mark[t] == s, t, 0)
        perm[s : s + 1, :] = rows[pl.ds(tile, 1), :]
    columns = perm[...].T
    def piece_copy(i, k):
        return remote(
            mine.at[i],
            weights.at[own_source * tb + i, pl.ds(pl.multiple_of(p * cl, cl), cl)],
            piece_send.at[k], w_recv.at[own_source, i, p],
            2 * z + 1 - x if k > n_pair else 2 * (seed(k) if k < n_pair else pair) + x, home,
        )

    def piece_sends(k):
        if k == 0:
            return home != p
        return home_here if k >= n_pair else True

    away = list(range(1, n_pair)) + [n_pair + 1, 0, n_pair]

    def send_pieces():
        mine_copy.wait()
        for k in away:
            for i in range(tb) if k == 0 else reversed(range(tb)):
                when(piece_sends(k), lambda i=i, k=k: piece_copy(i, k).start())

        @pl.when(home == p)
        def _():
            for i in range(tb):
                pltpu.make_async_copy(
                    pieces.at[i],
                    weights.at[own_source * tb + i, pl.ds(pl.multiple_of(p * cl, cl), cl)],
                    w_recv.at[own_source, i, p],
                ).start()

    def chunk(j, i, at):
        part = weights.at[j * tb + i, pl.ds(pl.multiple_of(at * cl, cl), cl)]
        return part, w_recv.at[j, i, at]

    def arrive(j, i, at):
        part, recv = chunk(j, i, at)
        pltpu.make_async_copy(part, part, recv).wait()

    def along_z(j, i, at, k, other=0):
        part, recv = chunk(j, i, at)
        return remote(
            part, part, z_send.at[(k or n_pair) if other else 0], recv, 2 * (seed(k) if k else pair) + x, p
        )

    def along_x(j, i, at):
        part, recv = chunk(j, i, at)
        return remote(part, part, x_send.at[0], recv, 2 * z + 1 - x, p)

    def crosses_early(i, dd):
        return dd > 0 and i % 2 == 0

    def onward(at_line, j, i, dd, at):
        copies = []
        if at_line == 2 or (at_line == 0 and dd):
            copies.append(along_z(j, i, at, 0))
        if (at_line == 0 and dd) or at_line == 1 or (at_line > 1 and not crosses_early(i, dd)):
            copies.append(along_x(j, i, at))
        return copies

    def onward_other(at_line, j, i, at):
        if at_line == 0:
            return [along_z(j, i, at, m, 1) for m in range(1, n_pair)]
        return [along_z(j, i, at, 0, 1)]

    def relay(at_line, chunks, other=False):
        for jj in range(g):
            j, zs, on_line = source(jj)
            if on_line is other:
                continue

            def body(j=j):
                for i, dd in chunks:
                    for half in range(2):
                        at = ((q + dd) % n_chips) * 2 + half
                        arrive(j, i, at)
                        if other:
                            copies = onward_other(at_line, j, i, at)
                        else:
                            copies = onward(at_line, j, i, dd, at)
                        for copy in copies:
                            copy.start()

            here = place(zs) == at_line
            if on_line is not True and on_line is not False:
                here = here & (jnp.logical_not(on_line) if other else on_line)
            if chunks:
                when(here, body)

    def sent(sem, count):
        if count:
            a = next(a for a in range(1, tp + 1) if count % a == 0 and count // a <= np_)
            part = weights.at[pl.ds(0, a), pl.ds(0, count // a * cl)]
            remote(part, part, sem, w_recv.at[0, 0, 0], 2 * z + 1 - x, p).wait_send()

    def relay_drain(at_line):
        across = [(i, dd) for i in range(tb) for dd in range(1, n_chips)]
        even = [1 for i, dd in across if crosses_early(i, dd)]
        in_plane, over, early = 2 * tb, 2 * len(across), 2 * len(even)
        along = {0: over, 1: 0, 2: in_plane + over, 3: 0}[at_line]
        beside = {0: over, 1: in_plane + over, 2: in_plane + over - early, 3: in_plane + over - early}[at_line]
        for jj in range(g):
            _, zs, on_line = source(jj)
            here = place(zs) == at_line

            def body():
                sent(z_send.at[0], along)
                sent(x_send.at[0], beside)

            def body_other():
                for m in range(1, n_pair) if at_line == 0 else (n_pair,):
                    sent(z_send.at[m], early)

            if on_line is not False:
                when(here if on_line is True else here & on_line, body)
            if on_line is not True and at_line % 2 == 0:
                when(here if on_line is False else here & jnp.logical_not(on_line), body_other)

    per = slots // PARTS

    def to_sibling(h):
        return remote(own[h], sib[h], sib_send.at[h], sib_recv.at[h], b, 2 * q + 1 - c)

    def gather(h):
        done = [
            jnp.dot(
                onehot[k * per * blk : (k + 1) * per * blk, :], lat[:, h * wide : (h + 1) * wide],
                preferred_element_type=f32,
            )
            for k in range(PARTS)
        ]
        for k in range(PARTS):
            own[h][k * per : (k + 1) * per] = done[k].astype(bf16).reshape(per, blk, wide)

    def share(h):
        to_sibling(h).start()

    def front(h):
        if h == 0:
            lat_copy.wait()
        gather(h)

    def build():
        iota = lax.broadcasted_iota(jnp.int32, (blk, mesh_dev), 1)
        for s in range(slots):
            hit = iota == columns[:, s : s + 1]
            onehot[s * blk : (s + 1) * blk, :] = jnp.where(hit, 1.0, 0.0).astype(bf16)

    pl.when(z < n_pair)(build)
    pl.when(z == 0)(lambda: front(0))
    pl.semaphore_wait(barrier, greetings)
    pl.when(z == 0)(lambda: share(0))
    send_pieces()

    @pl.when((z > 0) & (z < n_pair))
    def _():
        front(0)
        share(0)

    @pl.when(z >= n_pair)
    def _():
        build()
        front(0)
        share(0)

    front(1)
    share(1)

    def step_of(kk):
        return kk // tb, tb - 1 - kk % tb

    def tile_of(kk):
        jj, i = step_of(kk)
        return ((x + jj) % g) * tb + i

    def from_this_chip(h, t):
        return jnp.where(owners[t] == p, own[h][rank_of[t]], sib[h][rank_of[t]])

    def to_chip(h, d, kk):
        return remote(
            far.at[d - 1, kk, h], from_chip.at[d - 1, kk, h], chip_send.at[0], chip_recv.at[d - 1, kk],
            b, 2 * ((q + d) % n_chips) + c,
        )

    def chip_here(d, kk):
        part = from_chip.at[d - 1, kk]
        pltpu.make_async_copy(part, part, chip_recv.at[d - 1, kk]).wait()

    def send_far(h, kk):
        for d in range(1, n_chips):
            t = (2 * ((q + d) % n_chips) + c) * tp + tile_of(kk)
            far[d - 1, kk, h] = from_this_chip(h, t)
            to_chip(h, d, kk).start()

    def sibling_here(h):
        to_sibling(h).wait_recv()

    sibling_here(0)
    first = max(tp // 2, 1)
    for kk in range(first):
        send_far(0, kk)
    every = [(i, 0) for i in reversed(range(tb))]
    even = [(i, dd) for i in range(0, tb, 2) for dd in range(1, n_chips)]
    odd = [(i, dd) for i in range(1, tb, 2) for dd in range(1, n_chips)]
    early = {0: even, 2: every[:1]}
    late = {0: odd + every, 1: every[:1] + odd + every[1:], 2: odd + every[1:] + even, 3: every[:1] + odd}
    last = {1: even, 3: every[1:] + even}

    @pl.when(z != 0)
    def _():
        for k in early:
            relay(k, early[k])

    for copy in small[2:]:
        copy.wait()
    pltpu.make_async_copy(w_rows, w_rows, small_sem.at[4]).wait()
    pltpu.make_async_copy(w_both, w_both, wt_sem.at[0]).wait()
    w1, w2 = w_both.at[0], w_both.at[1]
    w_b1, w_b2, w_gain = (w_rows.at[k] for k in range(3))
    eye = jnp.where(
        lax.broadcasted_iota(jnp.int32, (width, width), 0)
        == lax.broadcasted_iota(jnp.int32, (width, width), 1), 1.0, 0.0,
    ).astype(bf16)
    w1t[...] = (0.5 * contract_last(eye, w1[...])).astype(bf16)
    w2e[EXT:, :] = contract_last(eye, w2[...]).astype(bf16)
    pad = EXT // 2
    scaled = jnp.concatenate(
        [w_out[...].astype(f32) * w_gain[...], jnp.zeros((pad - channels, width), f32)], axis=0
    )
    high, rest = split(scaled)
    mid, rest = split(rest)
    ones = jnp.full((pad, width), 1.0 / width, f32).astype(bf16)
    sums = contract_last(jnp.concatenate([high, mid, rest.astype(bf16), ones], axis=0), w2[...])
    mean_row = sums[3 * pad : 3 * pad + 1]
    head = sums[:pad] + sums[pad : 2 * pad] + sums[2 * pad : 3 * pad]
    head = head - jnp.sum(scaled, axis=1, keepdims=True) * mean_row
    head = jnp.where(lax.broadcasted_iota(jnp.int32, head.shape, 0) == channels, mean_row, head)
    high, rest = split(head)
    w2e[:pad, :] = high
    w2e[pad:EXT, :] = rest.astype(bf16)
    b2c = w_b2[...] - jnp.mean(w_b2[...], axis=1, keepdims=True)
    head_bias = jnp.sum(scaled * b2c, axis=1, keepdims=True)
    b2b[...] = jnp.transpose(jnp.broadcast_to(b2c, (128, width)))
    high, rest = split(jnp.transpose(jnp.broadcast_to(0.5 * w_b1[...], (128, width))))
    mid, rest = split(rest)
    lane = lax.broadcasted_iota(jnp.int32, (width, 128), 1)
    terms = (high.astype(f32), mid.astype(f32), rest)
    bias_columns = jnp.zeros((width, 128), f32)
    for k, term in enumerate(terms):
        bias_columns = jnp.where(lane == k, term, bias_columns)
    bft[:, blk:] = bias_columns.astype(bf16)
    diagonal = lax.broadcasted_iota(jnp.int32, (pad, channels), 0) == lax.broadcasted_iota(
        jnp.int32, (pad, channels), 1
    )
    bias = jnp.sum(jnp.where(diagonal, w_bo[...], 0.0), axis=1, keepdims=True)
    ones_columns = jnp.where(
        lax.broadcasted_iota(jnp.int32, (in_tile, 128), 1) < len(terms), 1.0, 0.0
    ).astype(bf16)

    sibling_here(1)
    for kk in range(first):
        send_far(1, kk)
    for kk in range(first, tp):
        for h in range(2):
            send_far(h, kk)
    @pl.when(z == 0)
    def _():
        for k in early:
            relay(k, early[k])

    for k in late:
        relay(k, late[k])
    relay(0, even, other=True)

    for kk in range(tp):
        jj, i = step_of(kk)
        j, zs, on_line = source(jj)
        if kk == min(1, tb - 1):
            for k in last:
                relay(k, last[k])
            relay(2, even, other=True)
        tile = tile_of(kk)
        t = p * tp + tile
        for d in range(1, n_chips):
            chip_here(d, kk)
        halves = []
        for h in range(2):
            value = from_this_chip(h, t)
            for d in range(1, n_chips):
                chip = 2 * ((q + n_chips - d) % n_chips)
                there = (owners[t] == chip) | (owners[t] == chip + 1)
                value = jnp.where(there, from_chip[d - 1, kk, h], value)
            halves.append(value)
        block = jnp.concatenate(halves, axis=1)

        def rest_arrives(j=j, i=i, zs=zs):
            for dd in range(n_chips):

                def wait(dd=dd):
                    for half in range(2):
                        arrive(j, i, ((q + dd) % n_chips) * 2 + half)

                when(place(zs) % 2 == 1 if crosses_early(i, dd) else True, wait)

        if on_line is not True:
            when(True if on_line is False else jnp.logical_not(on_line), rest_arrives)
        for r in range(2):
            at = slice(r * wide, (r + 1) * wide)
            bft[at, :blk] = contract_last(w1t[at, :], block).astype(bf16)
        cells = jnp.concatenate([weights[tile], ones_columns], axis=1)
        half_v = contract_last(bft[...], cells)
        hidden = (half_v * jnp.tanh(half_v) + half_v).astype(bf16)
        second = jnp.dot(w2e[...], hidden, preferred_element_type=f32)
        heads = second[:pad] + second[pad:EXT]
        mean = heads[channels : channels + 1]
        centred = second[EXT:] + jnp.concatenate([b2b[...]] * (in_tile // 128), axis=1) - mean
        variance = jnp.sum(centred * centred, axis=0, keepdims=True) * (1.0 / width)
        result = (heads + head_bias) * lax.rsqrt(variance + 1e-05) + bias
        at = pl.multiple_of(tile * in_tile, in_tile)
        for ch in range(channels):
            out[ch, :, pl.ds(at, in_tile)] = result[ch : ch + 1]

    def pieces_sent(k):
        return remote(mine, mine, piece_send.at[k], w_recv.at[0, 0, 0], 2 * z + 1 - x, home)

    for k in away:
        when(piece_sends(k), lambda k=k: pieces_sent(k).wait_send())
    for h in range(2):
        to_sibling(h).wait_send()
    if n_chips > 1:
        remote(far, far, chip_send.at[0], chip_recv.at[0, 0], b, 2 * q + 1 - c).wait_send()
    for k in range(4):
        relay_drain(k)


def solution(mesh):
    nb, np_ = mesh.shape["band"], mesh.shape["patch"]

    def body(
        latents, owners, block_rows, pieces, w_first, b_first, w_second, b_second, gain, w_out, b_out
    ):
        tiles, blk = block_rows.shape
        cl, channels = pieces.shape[1], w_out.shape[1]
        mesh_dev, width = latents.shape[1:]
        n_chips, tb, tp = np_ // 2, tiles // nb, tiles // np_
        g = tp // tb
        n_z = nb // 2
        slots = tiles // 2
        far = max(n_chips - 1, 1)
        hbm = pl.BlockSpec(memory_space=pltpu.HBM)
        bf16 = jnp.bfloat16
        dma = pltpu.SemaphoreType.DMA
        result = pl.pallas_call(
            functools.partial(kernel, nb, np_, tiles, blk, cl, slots),
            out_shape=pltpu.VMEM((channels, 1, tp * np_ * cl), jnp.float32),
            in_specs=[hbm] * 11,
            out_specs=pl.BlockSpec(memory_space=pltpu.VMEM),
            scratch_shapes=[
                pltpu.SMEM((tiles,), jnp.int32),
                pltpu.VMEM((tiles, blk), jnp.int32),
                pltpu.VMEM((3, 1, width), jnp.float32),
                pltpu.VMEM((channels, width), bf16),
                pltpu.VMEM((1, channels), jnp.float32),
                pltpu.VMEM((mesh_dev, width), bf16),
                pltpu.VMEM((2,) + w_first.shape[1:], bf16),
                pltpu.VMEM((tb, cl, blk), bf16),
                pltpu.VMEM((blk, blk), jnp.int32),
                pltpu.VMEM((slots * blk, mesh_dev), bf16),
            ]
            + [pltpu.VMEM((slots, blk, width // 2), bf16)] * 4
            + [
                pltpu.VMEM((far, tp, 2, blk, width // 2), bf16),
                pltpu.VMEM((far, tp, 2, blk, width // 2), bf16),
                pltpu.VMEM((tp, np_ * cl, blk), bf16),
                pltpu.VMEM((width, width), bf16),
                pltpu.VMEM((EXT + width, width), bf16),
                pltpu.VMEM((width, 128), jnp.float32),
                pltpu.VMEM((width, blk + 128), bf16),
                pltpu.SMEM((tiles,), jnp.int32),
                dma((5,)),
                dma((1,)),
                dma((1,)),
                dma((1,)),
                dma((n_z // 2 + 2,)),
                dma((g, tb, np_)),
                dma((n_z // 2 + 1,)),
                dma((1,)),
                dma((2,)),
                dma((2,)),
                dma((1,)),
                dma((far, tp)),
            ],
            compiler_params=pltpu.CompilerParams(collective_id=0, has_side_effects=True),
            name="decode",
        )(
            owners, block_rows, b_first, b_second, gain, w_out[0], b_out,
            latents[0], pieces, w_first[0], w_second[0],
        )
        return jnp.transpose(result, (1, 0, 2))

    return jax.shard_map(
        body,
        mesh=mesh,
        in_specs=(
            P("band", "patch", None),
            P(),
            P(),
            P("band", "patch", None),
            P("band", None, None),
            P("band", None),
            P("band", None, None),
            P("band", None),
            P("band", None),
            P("band", None, None),
            P("band", None),
        ),
        out_specs=P("band", None, "patch"),
        check_vma=False,
    )
```
